512 devices in a mesh: gx: 16 (over y, core), gy: 4 (over x), gz: 8 (over z).
Axes of the slice: x: 4, y: 8, z: 8, core: 2. Of those that a mesh axis runs over, the one named last changes fastest.
Arguments:
- fractions: float32 [3, 16, 8, 16, 128], P(None, 'gx', 'gy', 'gz'), may hold values from 0 to 1
- polarizability: float32 [16, 8, 16, 128], P('gx', 'gy', 'gz'), may hold values from 0.5 to 2
- occupancy: int32 [16, 8, 16, 128], P('gx', 'gy', 'gz'), may hold values 0 or 1
- pair_mask: int32 [16, 8, 16, 27], P('gx', 'gy', 'gz'), may hold values from 0 to 1, as said below
- perm_field: float32 [6, 16, 8, 16, 128], P(None, 'gx', 'gy', 'gz'), may hold values from -6 to 6
- history: float32 [6, 6, 16, 8, 16, 128], P(None, None, 'gx', 'gy', 'gz'), may hold values from -12 to 12
Outputs:
- induced: float32 [6, 16, 8, 16, 128], P(None, 'gx', 'gy', 'gz')
- change: float32 [], replicated
The draws below stay inside these ranges and needn't reach their ends.
Inputs may be any that keep to these rules, and one draw needn't show every extreme that they name: pair_mask[t, k] equals pair_mask at tile t + offset(k) for the opposite offset 26 - k (periodic); pair_mask[t, 13] (the tile itself) is 1.
All inputs are finite; a program needn't handle non-finite values. No bound on the sum of `occupancy` on one device may be relied on, other than what follows from the above.
Results may differ from the reference program's by a relative error of at most 0.0003.
Values sent between devices are 32-bit elements; how exact they have to be, the bound alone decides.
A program may use at most 64 MiB of HBM per device.

```python
import math
import jax
import jax.numpy as jnp
from jax import lax

TILE = 128
HIST = 6
TILES_X = 1
TILES_Y = 2
TILES_Z = 2
BOX_X = 16
BOX_Y = 8
BOX_Z = 16


def draw_history(key, part):
    subkeys = jax.random.split(key, 6)
    full_shape = (6, BOX_X, BOX_Y, BOX_Z, TILE)
    block_counts = (BOX_X // TILES_X, BOX_Y // TILES_Y, BOX_Z // TILES_Z)
    frequency_table = jax.random.uniform(subkeys[4], block_counts, jnp.float32, 0.25, 2.2)
    index_x = jnp.arange(BOX_X) // TILES_X
    index_y = jnp.arange(BOX_Y) // TILES_Y
    index_z = jnp.arange(BOX_Z) // TILES_Z
    frequency = frequency_table[index_x[:, None, None], index_y[None, :, None], index_z[None, None, :]]
    step_index = jnp.arange(HIST, dtype=jnp.float32).reshape(HIST, 1, 1, 1, 1, 1)
    phase_angle = step_index * frequency[None, None, :, :, :, None]
    baseline = jax.random.normal(subkeys[0], full_shape, jnp.float32)
    cosine_part = jax.random.normal(subkeys[1], full_shape, jnp.float32)
    sine_part = jax.random.normal(subkeys[2], full_shape, jnp.float32)
    jitter = 0.2 * jax.random.normal(subkeys[3], (HIST,) + full_shape, jnp.float32)
    amplitude = jnp.exp(jax.random.uniform(subkeys[5], (1, 1, BOX_X, BOX_Y, BOX_Z, 1), jnp.float32, -0.7, 0.7))
    values = amplitude * (baseline[None] + jnp.cos(phase_angle) * cosine_part[None] + jnp.sin(phase_angle) * sine_part[None] + jitter)
    return jnp.clip(values, -12.0, 12.0).astype(jnp.float32)


def draw_pair_mask(key, part):
    coin_flips = jax.random.randint(key, (BOX_X, BOX_Y, BOX_Z, 27), 0, 4)
    one_side = (coin_flips > 0).astype(jnp.int32)
    columns = []
    for offset in range(27):
        along_x = offset // 9 - 1
        along_y = offset // 3 % 3 - 1
        along_z = offset % 3 - 1
        if offset == 13:
            columns.append(jnp.ones_like(one_side[..., offset]))
        else:
            mirror = jnp.roll(one_side[..., 26 - offset], shift=(-along_x, -along_y, -along_z), axis=(0, 1, 2))
            columns.append(one_side[..., offset] * mirror)
    return jnp.stack(columns, -1).astype(jnp.int32)


def with_ends(drawn, own_key, low, top_value):
    extent = drawn.shape
    index_at = [jax.random.randint(jax.random.fold_in(own_key, axis), (), 0, extent[axis]) for axis in range(len(extent))]
    drawn = drawn.at[tuple(index_at)].set(low)
    longest = extent.index(max(extent))
    index_at[longest] = (index_at[longest] + 1) % extent[longest]
    return drawn.at[tuple(index_at)].set(top_value)


def shard_levels(key, extent, cuts, least, high):
    loudness = 1.0
    for axis_at, blocks in cuts:
        draws = jax.random.uniform(jax.random.fold_in(jax.random.fold_in(key, 6), axis_at), (blocks,), jnp.float32, least / len(cuts), high / len(cuts))
        loudness = loudness * jnp.repeat(jnp.exp(draws), extent[axis_at] // blocks).reshape((-1,) + (1,) * (len(extent) - 1 - axis_at))
    return loudness


def scatter_about(key, dims, width, limit, pieces=(), held_as=jnp.bfloat16):
    result = jax.random.normal(key, dims, jnp.float32) * width
    if len(pieces) > 0:
        result = shard_levels(key, dims, pieces, -0.22, 0.18) * result
    return jnp.clip(result, min=-limit, max=limit).astype(held_as)


def setup_inputs(seed: int = 0) -> dict:
    key_of = jax.random.split(jax.random.key(seed), 7)
    fractions = jnp.clip(1.0 * jax.random.uniform(key_of[0], (3, BOX_X, BOX_Y, BOX_Z, TILE), jnp.float32) ** shard_levels(key_of[0], (3, BOX_X, BOX_Y, BOX_Z, TILE), ((1, 16), (2, 4), (3, 8)), -0.2, 0.2), 0.0, 1.0)
    polarizability = jnp.clip(jnp.exp(math.log(2.0) - 1.3862944 * jax.random.uniform(key_of[1], (BOX_X, BOX_Y, BOX_Z, TILE), jnp.float32) ** shard_levels(key_of[1], (BOX_X, BOX_Y, BOX_Z, TILE), ((0, 16), (1, 4), (2, 8)), -0.2, 0.2)), 0.5, 2.0)
    occupancy = with_ends((jax.random.randint(key_of[2], (BOX_X, BOX_Y, BOX_Z, TILE), 0, 8) < 7).astype(jnp.int32), jax.random.fold_in(key_of[2], 1), 0, 1)
    pair_mask = draw_pair_mask(jax.random.fold_in(key_of[6], 71), 0)
    perm_field = scatter_about(key_of[4], (6, BOX_X, BOX_Y, BOX_Z, TILE), 1.0, 6.0, ((1, 16), (2, 4), (3, 8)), jnp.float32)
    history = draw_history(jax.random.fold_in(key_of[6], 71), 0)
    return {"fractions": fractions, "polarizability": polarizability, "occupancy": occupancy, "pair_mask": pair_mask, "perm_field": perm_field, "history": history}


CELL_EDGE = 10.0
SOFTENING = 0.3
THOLE_DAMP = 0.39
RELAXATION = 0.7

def pair_field(target, source, moment, offset_vec, itself, allowed):
    displace = [(offset_vec[axis_num] + source[axis_num][:, None, :] - target[axis_num][:, :, None]) * CELL_EDGE for axis_num in range(3)]
    dist_sq = displace[0] * displace[0] + displace[1] * displace[1] + displace[2] * displace[2] + SOFTENING
    inv_cube = lax.rsqrt(dist_sq) / dist_sq
    thole_arg = dist_sq * jnp.sqrt(dist_sq) * lax.rsqrt(target[3][:, :, None] * source[3][:, None, :])
    damping = jnp.exp(-THOLE_DAMP * thole_arg)
    lambda_three = 1.0 - damping
    lambda_five = 1.0 - (1.0 + THOLE_DAMP * thole_arg) * damping
    slots = target.shape[-1]
    self_pair = jnp.logical_and(itself, jnp.eye(slots, dtype=bool))
    weight = jnp.where(self_pair, 0.0, allowed[:, None, None])
    radial = 3.0 * lambda_five * inv_cube / dist_sq * weight
    direct = lambda_three * inv_cube * weight
    fields = []
    for which_set in range(moment.shape[0] // 3):
        parts = [moment[3 * which_set + axis_num][:, None, :] for axis_num in range(3)]
        project = displace[0] * parts[0] + displace[1] * parts[1] + displace[2] * parts[2]
        for axis_num in range(3):
            fields.append(lax.optimization_barrier(jnp.sum(radial * project * displace[axis_num] - direct * parts[axis_num], axis=-1)))
    return jnp.stack(fields)

def slab_field(geometry_pad, moment_pad, allowed_slab, slab_index):
    width_y = geometry_pad.shape[2] - 2
    width_z = geometry_pad.shape[3] - 2
    slots = geometry_pad.shape[4]
    rows = moment_pad.shape[0]
    zero = jnp.zeros((), jnp.int32)
    one = jnp.ones((), jnp.int32)
    first_x = (jnp.asarray(slab_index) + 1).astype(jnp.int32)
    target = lax.dynamic_slice(geometry_pad, (zero, first_x, one, one, zero), (4, 1, width_y, width_z, slots)).reshape(4, width_y * width_z, slots)

    def offset_step(offset, summed):
        offset = jnp.asarray(offset).astype(jnp.int32)
        along_x = offset // 9 - 1
        along_y = offset // 3 % 3 - 1
        along_z = offset % 3 - 1
        starts = (zero, first_x + along_x, one + along_y, one + along_z, zero)
        source = lax.dynamic_slice(geometry_pad, starts, (4, 1, width_y, width_z, slots)).reshape(4, width_y * width_z, slots)
        moment = lax.dynamic_slice(moment_pad, starts, (rows, 1, width_y, width_z, slots)).reshape(rows, width_y * width_z, slots)
        allowed = lax.dynamic_index_in_dim(allowed_slab, offset, 2, keepdims=False).reshape(-1).astype(jnp.float32)
        offset_vec = jnp.stack([along_x, along_y, along_z]).astype(jnp.float32)
        return summed + pair_field(target, source, moment, offset_vec, offset == 13, allowed)
    summed = lax.fori_loop(0, 27, offset_step, jnp.zeros((rows, width_y * width_z, slots), jnp.float32))
    return summed.reshape(rows, width_y, width_z, slots)

def wrap_pad(values):
    return jnp.pad(values, ((0, 0), (1, 1), (1, 1), (1, 1), (0, 0)), mode='wrap')

def box_field(geometry_pad, moment, pair_mask):
    moment_pad = wrap_pad(moment)

    def one_slab(slab_index):
        allowed_slab = lax.dynamic_index_in_dim(pair_mask, slab_index, 0, keepdims=False)
        return slab_field(geometry_pad, moment_pad, allowed_slab, slab_index)
    slabs = lax.map(one_slab, jnp.arange(pair_mask.shape[0], dtype=jnp.int32))
    return jnp.moveaxis(slabs, 0, 1)

def fit_coefficients(gram_matrix):
    past_count = gram_matrix.shape[0] - 1
    gram_past = gram_matrix[:past_count, :past_count]
    gram_next = gram_matrix[:past_count, past_count]
    ridge_term = 0.001 * jnp.trace(gram_past) / past_count + 1.0
    factor = jnp.linalg.cholesky(gram_past + ridge_term * jnp.eye(past_count, dtype=jnp.float32))
    return jax.scipy.linalg.cho_solve((factor, True), gram_next)

def reference(fractions, polarizability, occupancy, pair_mask, perm_field, history):
    filled = occupancy.astype(jnp.float32)
    geometry = jnp.concatenate([fractions, polarizability[None]], 0)
    masked = history * filled
    flat_hist = masked.reshape(masked.shape[0], -1)
    gram_matrix = jnp.dot(flat_hist, flat_hist.T, precision=lax.Precision.HIGHEST)
    coeffs = fit_coefficients(gram_matrix)
    predicted = jnp.tensordot(coeffs, masked[1:], axes=1, precision=lax.Precision.HIGHEST)
    geometry_pad = wrap_pad(geometry)
    scaled = RELAXATION * filled * polarizability
    field_one = box_field(geometry_pad, predicted, pair_mask)
    dipole_one = (1.0 - RELAXATION) * predicted + scaled * (perm_field + field_one)
    field_two = box_field(geometry_pad, dipole_one, pair_mask)
    induced = (1.0 - RELAXATION) * dipole_one + scaled * (perm_field + field_two)
    update = induced - dipole_one
    change = jnp.sqrt(jnp.sum(update * update) / (jnp.sum(induced * induced) + 1.0))
    return (induced, change)
```

```python
import math

import jax
import jax.numpy as jnp
from jax import lax
from jax.experimental import pallas as pl
from jax.experimental.pallas import tpu as pltpu
from jax.sharding import PartitionSpec as P

AXES = ("gx", "gy", "gz")
ORDER = ("gx", "gz", "gy")
MESH = pl.DeviceIdType.MESH
F32 = jnp.float32
BF16 = jnp.bfloat16
LANES = 128
DIRECTIONS = [
    (dx, dy, dz)
    for dx in (-1, 0, 1)
    for dy in (-1, 0, 1)
    for dz in (-1, 0, 1)
    if (dx, dy, dz) != (0, 0, 0)
]
CELL_EDGE = 10.0
SOFTENING = 0.3
THOLE_DAMP = 0.39
RELAXATION = 0.7
LN2 = math.log(2.0)
DAMP_ROOT = math.sqrt(THOLE_DAMP / LN2)
RECEIVERS = [(ry, rz) for ry in (0, 1) for rz in (0, 1)]


def away(sizes, axis, step):
    return lax.rem(lax.axis_index(axis) + (step + sizes[axis]), sizes[axis])


def neighbour(sizes, direction):
    return {axis: away(sizes, axis, step) for axis, step in zip(AXES, direction) if step != 0}


def sent_part(step):
    return {0: pl.ds(1, 2), 1: pl.ds(2, 1), -1: pl.ds(1, 1)}[step]


def landing_part(step):
    return {0: pl.ds(1, 2), 1: pl.ds(0, 1), -1: pl.ds(3, 1)}[step]


def halo_copies(sizes, buf, send_sem, recv_sem):
    copies = []
    for number, direction in enumerate(DIRECTIONS):
        dx, dy, dz = direction
        copies.append(
            pltpu.make_async_remote_copy(
                src_ref=buf.at[pl.ds(1, 1), sent_part(dy), sent_part(dz)],
                dst_ref=buf.at[pl.ds(1 - dx, 1), landing_part(dy), landing_part(dz)],
                send_sem=send_sem.at[number],
                recv_sem=recv_sem.at[number],
                device_id=neighbour(sizes, direction),
                device_id_type=MESH,
            )
        )
    return copies


def line_copies(sizes, axis, buf, send_sem, recv_sem):
    me = lax.axis_index(axis)
    copies = []
    for step in range(1, sizes[axis]):
        copies.append(
            pltpu.make_async_remote_copy(
                src_ref=buf.at[me],
                dst_ref=buf.at[me],
                send_sem=send_sem.at[step],
                recv_sem=recv_sem.at[step],
                device_id={axis: away(sizes, axis, step)},
                device_id_type=MESH,
            )
        )
    return copies


def kernel(
    sizes,
    frac_ref,
    pol_ref,
    occ_ref,
    mask_ref,
    perm_ref,
    hist_ref,
    out_ref,
    change_ref,
    geo,
    past,
    masked,
    moved_one,
    moved_two,
    perm_tiles,
    scaled_tiles,
    place,
    ends,
    columns,
    pairs,
    feats,
    *rest,
):
    lines_one, lines_two = rest[0:3], rest[3:6]
    geo_sems, past_sems, dip_sems = rest[6:8], rest[8:10], rest[10:12]
    sems_one = [rest[12 + 2 * n : 14 + 2 * n] for n in range(3)]
    sems_two = [rest[18 + 2 * n : 20 + 2 * n] for n in range(3)]

    barrier = pltpu.get_barrier_semaphore()
    greeted = [neighbour(sizes, direction) for direction in DIRECTIONS]
    for axis in AXES:
        greeted += [{axis: away(sizes, axis, step)} for step in range(2, sizes[axis] - 1)]
    for device in greeted:
        pl.semaphore_signal(barrier, inc=1, device_id=device, device_id_type=MESH)

    lane = lax.broadcasted_iota(jnp.int32, (1, LANES), 1)
    sub = lax.broadcasted_iota(jnp.int32, (8, LANES), 0)

    filled = occ_ref[...].astype(F32)
    filled_rows = jnp.concatenate([filled] * 6, axis=0)
    for h in range(6):
        masked[h] = hist_ref[h] * filled_rows
    for tile, (ry, rz) in enumerate(RECEIVERS):
        own = (1, 1 + ry, 1 + rz)
        weight = jnp.broadcast_to(
            RELAXATION * occ_ref[pl.ds(tile, 1), :].astype(F32) * pol_ref[pl.ds(tile, 1), :],
            (8, LANES),
        )
        scaled_tiles[tile] = jnp.where(lax.rem(sub, 4) == 3, 0.0, weight)
        perm_tiles[tile] = jnp.zeros((8, LANES), F32)
        for which in range(2):
            geo[own + (pl.ds(4 * which, 3),)] = frac_ref[pl.ds(tile, 3, stride=4), :]
            geo[own + (pl.ds(4 * which + 3, 1),)] = pol_ref[pl.ds(tile, 1), :]
            perm_tiles[tile, pl.ds(4 * which, 3), :] = perm_ref[
                pl.ds(12 * which + tile, 3, stride=4), :
            ]
        for h in range(5):
            past[own + (pl.ds(6 * h, 6),)] = masked[h + 1, pl.ds(tile, 6, stride=4), :]
        past[own + (pl.ds(30, 2),)] = jnp.zeros((2, LANES), F32)

    row = jnp.zeros((1, LANES), F32)
    for a in range(6):
        for b in range(a, 6):
            product = masked[a] * masked[b]
            folded = product[0:8] + product[8:16] + product[16:24]
            value = jnp.sum(jnp.sum(folded, axis=0, keepdims=True), axis=1, keepdims=True)
            row = jnp.where(lane == 6 * a + b, value, row)

    def send_line(number, bufs, sems, values):
        axis = ORDER[number]
        bufs[number][lax.axis_index(axis)] = values
        copies = line_copies(sizes, axis, bufs[number], *sems[number])
        for copy in copies:
            copy.start()
        return copies

    def total_line(number, bufs, copies):
        for copy in copies:
            copy.wait_recv()
        return jnp.sum(bufs[number][...], axis=0)

    pl.semaphore_wait(barrier, len(greeted))

    started = []
    line = send_line(0, lines_one, sems_one, row)
    started += line
    geo_copies = halo_copies(sizes, geo, *geo_sems)
    for copy in geo_copies:
        copy.start()
    past_copies = halo_copies(sizes, past, *past_sems)

    row = total_line(0, lines_one, line)
    line = send_line(1, lines_one, sems_one, row)
    started += line
    for copy in past_copies:
        copy.start()
    started += geo_copies + past_copies

    for copy in geo_copies:
        copy.wait_recv()

    slab_row = lax.broadcasted_iota(jnp.int32, (LANES, LANES), 0)
    kind = lax.rem(slab_row, 4)
    tile_y = slab_row // 32
    tile_z = lax.rem(slab_row // 8, 4)
    for sx in range(3):
        shift = jnp.where(
            kind == 0,
            jnp.float32(sx - 1.5),
            jnp.where(kind == 1, (tile_y - 2).astype(F32), (tile_z - 2).astype(F32)),
        )
        slab = geo[sx].reshape(LANES, LANES)
        at = (slab + shift) * CELL_EDGE
        place[sx] = jnp.where(kind == 3, DAMP_ROOT * lax.rsqrt(slab), at)
        ends[sx] = jnp.where(kind == 3, 1.0, at)
        columns[sx] = jnp.transpose(place[sx])

    lane16 = lax.broadcasted_iota(jnp.int32, (16, LANES), 1)
    sub16 = lax.broadcasted_iota(jnp.int32, (16, LANES), 0)

    def pair_block(step, carry):
        sx = step // 8
        block = lax.rem(step, 8)
        first = pl.multiple_of(block * 16, 16)
        cols = columns[sx, pl.ds(first, 16), :]
        apart = jnp.logical_or(sub16 + first != lane16, sx != 1)
        for sy in range(4):
            for sz in range(4):
                at = 8 * (4 * sy + sz)
                source = [
                    jnp.broadcast_to(cols[:, at + n : at + n + 1], (16, LANES)) for n in range(4)
                ]
                for tile, (ry, rz) in enumerate(RECEIVERS):
                    ky, kz = sy - ry, sz - rz
                    if not (0 <= ky <= 2 and 0 <= kz <= 2):
                        continue
                    mine = 8 * (4 * (ry + 1) + rz + 1)
                    d = [source[n] - place[1, pl.ds(mine + n, 1), :] for n in range(3)]
                    damp = source[3] * place[1, pl.ds(mine + 3, 1), :]
                    offset = 9 * sx + 3 * ky + kz
                    allowed = 3.0 * mask_ref[tile, offset].astype(F32)
                    dist = d[0] * d[0] + d[1] * d[1] + d[2] * d[2] + SOFTENING
                    root = lax.rsqrt(dist)
                    inverse = root * root
                    cube = root * inverse * allowed
                    if ky == 1 and kz == 1:
                        cube = jnp.where(apart, cube, 0.0)
                    power = dist * dist * root * damp
                    fade = jnp.exp2(-power)
                    three = 1.0 - fade
                    five = three - (power * LN2) * fade
                    direct = three * cube
                    radial = five * (inverse * cube)
                    base = offset * 256 + first
                    for part, value in ((0, radial), (128, direct)):
                        high = value.astype(BF16)
                        low = (value - high.astype(F32)).astype(BF16)
                        rows = pl.ds(pl.multiple_of(base + part, 16), 16)
                        pairs[tile, rows, pl.ds(0, 128)] = high
                        pairs[tile, rows, pl.ds(128, 128)] = low
        return carry

    lax.fori_loop(0, 12, pair_block, 0)
    row = total_line(1, lines_one, line)
    line = send_line(2, lines_one, sems_one, row)
    started += line
    lax.fori_loop(12, 24, pair_block, 0)
    row = total_line(2, lines_one, line)

    def entry(a, b):
        return jnp.sum(
            jnp.where(lane == 6 * min(a, b) + max(a, b), row, 0.0), axis=1, keepdims=True
        )

    gram = {(a, b): entry(a, b) for a in range(6) for b in range(a, 6) if a < 5}
    trace = gram[0, 0] + gram[1, 1] + gram[2, 2] + gram[3, 3] + gram[4, 4]
    ridge = 0.001 * trace / 5.0 + 1.0
    low = {}
    scale = []
    half = []
    for a in range(5):
        pivot = gram[a, a] + ridge
        for c in range(a):
            pivot = pivot - low[a, c] * low[a, c]
        scale.append(lax.rsqrt(pivot))
        for b in range(a + 1, 5):
            value = gram[a, b]
            for c in range(a):
                value = value - low[a, c] * low[b, c]
            low[b, a] = value * scale[a]
        value = gram[a, 5]
        for c in range(a):
            value = value - low[a, c] * half[c]
        half.append(value * scale[a])
    coeffs = [None] * 5
    for a in reversed(range(5)):
        value = half[a]
        for b in range(a + 1, 5):
            value = value - low[b, a] * coeffs[b]
        coeffs[a] = value * scale[a]
    coeffs = [jnp.broadcast_to(value, (8, LANES))[0:6] for value in coeffs]

    for copy in past_copies:
        copy.wait_recv()

    first_set = sub < 4

    def write_feats(sx, s, tile_ref):
        whole = tile_ref[...]
        near = ends[sx, pl.ds(pl.multiple_of(8 * s, 8), 8), :]
        multipliers = []
        along = None
        for b in range(3):
            both = jnp.where(first_set, whole[b : b + 1], whole[4 + b : 5 + b])
            multipliers.append(both)
            term = near[b : b + 1] * both
            along = term if along is None else along + term
        multipliers.append(along)
        parts = [near * value for value in multipliers]
        flat = jnp.zeros((8, LANES), F32)
        for half_at in range(2):
            value = jnp.concatenate(parts[2 * half_at : 2 * half_at + 2], axis=0)
            other = jnp.concatenate(
                [flat, whole * (-1.0 / 3.0) if half_at == 1 else flat], axis=0
            )
            for piece in range(3):
                rows = pl.ds(32 * piece + 16 * half_at, 16)
                kept = value.astype(BF16)
                feats[sx, s, rows, pl.ds(0, 128)] = kept
                value = value - kept.astype(F32)
                kept = other.astype(BF16)
                feats[sx, s, rows, pl.ds(128, 128)] = kept
                other = other - kept.astype(F32)

    def predict(number, carry):
        sx, s = number // 16, lax.rem(number, 16)
        sy, sz = s // 4, lax.rem(s, 4)
        total = None
        for h in range(5):
            term = coeffs[h] * past[sx, sy, sz, pl.ds(6 * h, 6), :]
            total = term if total is None else total + term
        moved_one[sx, sy, sz] = jnp.zeros((8, LANES), F32)
        moved_one[sx, sy, sz, pl.ds(0, 3), :] = total[0:3]
        moved_one[sx, sy, sz, pl.ds(4, 3), :] = total[3:6]
        write_feats(sx, s, moved_one.at[sx, sy, sz])
        return carry

    lax.fori_loop(0, 48, predict, 0)

    def field(tile):
        ry, rz = RECEIVERS[tile]
        summed = None
        for kx in range(3):
            lhs = jnp.concatenate(
                [feats[kx, 4 * (ry + ky) + rz + kz] for ky in range(3) for kz in range(3)], axis=1
            )
            part = jnp.dot(
                lhs, pairs[tile, pl.ds(2304 * kx, 2304), :], preferred_element_type=F32
            )
            summed = part if summed is None else summed + part
        both = summed[:, 0:128] + summed[:, 128:256]
        out = both[0:32] + both[32:64] + both[64:96]
        mine = 8 * (4 * (ry + 1) + rz + 1)
        here = ends[1, pl.ds(mine, 8), :]
        value = out[24:32]
        for b in range(3):
            value = value - here[b : b + 1] * out[8 * b : 8 * b + 8]
        shared = jnp.where(first_set, value[3:4], value[7:8])
        return value - here * shared

    def relaxed(tile, before):
        return (1.0 - RELAXATION) * before + scaled_tiles[tile] * (perm_tiles[tile] + field(tile))

    for tile, (ry, rz) in enumerate(RECEIVERS):
        moved_two[1, 1 + ry, 1 + rz] = relaxed(tile, moved_one[1, 1 + ry, 1 + rz])

    dip_copies = halo_copies(sizes, moved_two, *dip_sems)
    for copy in dip_copies:
        copy.start()
    started += dip_copies
    for copy in dip_copies:
        copy.wait_recv()

    def second(number, carry):
        sx, s = number // 16, lax.rem(number, 16)
        write_feats(sx, s, moved_two.at[sx, s // 4, lax.rem(s, 4)])
        return carry

    lax.fori_loop(0, 48, second, 0)

    changed = jnp.zeros((8, LANES), F32)
    size = jnp.zeros((8, LANES), F32)
    for tile, (ry, rz) in enumerate(RECEIVERS):
        before = moved_two[1, 1 + ry, 1 + rz]
        after = relaxed(tile, before)
        out_ref[pl.ds(tile, 3, stride=4), :] = after[0:3]
        out_ref[pl.ds(12 + tile, 3, stride=4), :] = after[4:7]
        update = after - before
        changed = changed + update * update
        size = size + after * after

    def whole_sum(value):
        return jnp.sum(jnp.sum(value, axis=0, keepdims=True), axis=1, keepdims=True)

    row = jnp.where(lane == 0, whole_sum(changed), jnp.where(lane == 1, whole_sum(size), 0.0))
    for number in range(3):
        line = send_line(number, lines_two, sems_two, row)
        started += line
        row = total_line(number, lines_two, line)
    top = jnp.sum(jnp.where(lane == 0, row, 0.0), axis=1, keepdims=True)
    bottom = jnp.sum(jnp.where(lane == 1, row, 0.0), axis=1, keepdims=True)
    change_ref[...] = jnp.broadcast_to(jnp.sqrt(top / (bottom + 1.0)), (1, LANES))

    for copy in started:
        copy.wait_send()


def on_device(sizes, fractions, polarizability, occupancy, pair_mask, perm_field, history):
    vmem = pl.BlockSpec(memory_space=pltpu.VMEM)
    smem = pl.BlockSpec(memory_space=pltpu.SMEM)
    dma = pltpu.SemaphoreType.DMA
    line_bufs = [pltpu.VMEM((sizes[axis], 1, LANES), F32) for axis in ORDER]
    line_sems = []
    for axis in ORDER:
        line_sems += [dma((sizes[axis],)), dma((sizes[axis],))]
    scratch = [
        pltpu.VMEM((3, 4, 4, 8, LANES), F32),
        pltpu.VMEM((3, 4, 4, 32, LANES), F32),
        pltpu.VMEM((6, 24, LANES), F32),
        pltpu.VMEM((3, 4, 4, 8, LANES), F32),
        pltpu.VMEM((3, 4, 4, 8, LANES), F32),
        pltpu.VMEM((4, 8, LANES), F32),
        pltpu.VMEM((4, 8, LANES), F32),
        pltpu.VMEM((3, LANES, LANES), F32),
        pltpu.VMEM((3, LANES, LANES), F32),
        pltpu.VMEM((3, LANES, LANES), F32),
        pltpu.VMEM((4, 27 * 256, 256), BF16),
        pltpu.VMEM((3, 16, 96, 256), BF16),
    ]
    scratch += line_bufs + line_bufs + [dma((26,))] * 6 + line_sems + line_sems
    induced, change = pl.pallas_call(
        lambda *refs: kernel(sizes, *refs),
        out_shape=(
            jax.ShapeDtypeStruct((24, LANES), F32),
            jax.ShapeDtypeStruct((1, LANES), F32),
        ),
        in_specs=[vmem, vmem, vmem, smem, vmem, vmem],
        out_specs=(vmem, vmem),
        scratch_shapes=scratch,
        compiler_params=pltpu.CompilerParams(
            collective_id=0, has_side_effects=True, vmem_limit_bytes=60 * 1024 * 1024
        ),
    )(
        fractions.reshape(12, LANES),
        polarizability.reshape(4, LANES),
        occupancy.reshape(4, LANES),
        pair_mask.reshape(4, 27),
        perm_field.reshape(24, LANES),
        history.reshape(6, 24, LANES),
    )
    return induced.reshape(6, 1, 2, 2, LANES), change[0, 0]


def solution(mesh):
    sizes = {axis: mesh.shape[axis] for axis in AXES}
    placed = (
        P(None, "gx", "gy", "gz", None),
        P("gx", "gy", "gz", None),
        P("gx", "gy", "gz", None),
        P("gx", "gy", "gz", None),
        P(None, "gx", "gy", "gz", None),
        P(None, None, "gx", "gy", "gz", None),
    )
    return jax.shard_map(
        lambda *args: on_device(sizes, *args),
        mesh=mesh,
        in_specs=placed,
        out_specs=(P(None, "gx", "gy", "gz", None), P()),
        check_vma=False,
    )
```

```python
import math

import jax
import jax.numpy as jnp
from jax import lax
from jax.experimental import pallas as pl
from jax.experimental.pallas import tpu as pltpu
from jax.sharding import PartitionSpec as P

AXES = ("gx", "gy", "gz")
FIRST_GROUPS = (("gx",), ("gz",), ("gy",))
LAST_GROUPS = (("gx",), ("gy", "gz"))
MESH = pl.DeviceIdType.MESH
F32 = jnp.float32
BF16 = jnp.bfloat16
LANES = 128
DIRECTIONS = [
    (dx, dy, dz)
    for dx in (-1, 0, 1)
    for dy in (-1, 0, 1)
    for dz in (-1, 0, 1)
    if (dx, dy, dz) != (0, 0, 0)
]
CELL_EDGE = 10.0
SOFTENING = 0.3
THOLE_DAMP = 0.39
RELAXATION = 0.7
LN2 = math.log(2.0)
DAMP_ROOT = math.sqrt(THOLE_DAMP / LN2)
RECEIVERS = [(ry, rz) for ry in (0, 1) for rz in (0, 1)]


SEMS = 8 + len(FIRST_GROUPS) + len(LAST_GROUPS)
VMEM_BYTES = 62 * 1000 * 1000


def away(sizes, axis, step):
    return lax.rem(lax.axis_index(axis) + (step + sizes[axis]), sizes[axis])


def neighbour(sizes, direction):
    return {axis: away(sizes, axis, step) for axis, step in zip(AXES, direction) if step != 0}


def sent_part(step):
    return {0: pl.ds(1, 2), 1: pl.ds(2, 1), -1: pl.ds(1, 1)}[step]


def landing_part(step):
    return {0: pl.ds(1, 2), 1: pl.ds(0, 1), -1: pl.ds(3, 1)}[step]


def remote(src, dst, sems, device):
    return pltpu.make_async_remote_copy(
        src_ref=src,
        dst_ref=dst,
        send_sem=sems[0],
        recv_sem=sems[1],
        device_id=device,
        device_id_type=MESH,
    )


class Batch:
    def __init__(self, copies, counted, sems, device):
        self.copies = copies
        self.whole = remote(counted, counted, sems, device)

    def start(self):
        for copy in self.copies:
            copy.start()

    def arrived(self):
        self.whole.wait_recv()

    def sent(self):
        self.whole.wait_send()


def halo_batch(sizes, buf, sems, same_slab):
    copies = []
    for direction in DIRECTIONS:
        dx, dy, dz = direction
        if (dx == 0) != same_slab:
            continue
        copies.append(
            remote(
                buf.at[pl.ds(1, 1), sent_part(dy), sent_part(dz)],
                buf.at[pl.ds(1 - dx, 1), landing_part(dy), landing_part(dz)],
                sems,
                neighbour(sizes, direction),
            )
        )
    counted = buf.at[1, pl.ds(0, 3)] if same_slab else buf.at[pl.ds(0, 2)]
    return Batch(copies, counted, sems, neighbour(sizes, (0, 0, 1)))


def tile_batch(sizes, buf, sems, tile, counted):
    ry, rz = RECEIVERS[tile]
    mine = buf.at[1, 1 + ry, 1 + rz]
    copies = []
    for dx in (-1, 0, 1):
        for dy, at_y in ((0, 1 + ry), (2 * ry - 1, 3 - 3 * ry)):
            for dz, at_z in ((0, 1 + rz), (2 * rz - 1, 3 - 3 * rz)):
                if (dx, dy, dz) != (0, 0, 0):
                    copies.append(
                        remote(
                            mine,
                            buf.at[1 - dx, at_y, at_z],
                            sems,
                            neighbour(sizes, (dx, dy, dz)),
                        )
                    )
    return Batch(copies, counted, sems, neighbour(sizes, (0, 0, 1)))


def group_steps(sizes, axes):
    steps = [()]
    for axis in axes:
        steps = [step + (n,) for step in steps for n in range(sizes[axis])]
    far = lambda step: sum(min(n, sizes[axis] - n) for n, axis in zip(step, axes))
    return sorted([step for step in steps if any(step)], key=far, reverse=True)


def group_batch(sizes, axes, buf, sems):
    me = 0
    for axis in axes:
        me = me * sizes[axis] + lax.axis_index(axis)
    copies = []
    for step in group_steps(sizes, axes):
        device = {axis: away(sizes, axis, n) for axis, n in zip(axes, step) if n != 0}
        copies.append(remote(buf.at[me], buf.at[me], sems, device))
    counted = buf.at[pl.ds(0, len(copies))]
    return me, Batch(copies, counted, sems, {axes[0]: away(sizes, axes[0], 1)})


def kernel(
    sizes,
    frac_hbm,
    pol_hbm,
    occ_hbm,
    mask_hbm,
    perm_hbm,
    hist_hbm,
    out_ref,
    change_ref,
    frac_ref,
    pol_ref,
    occ_ref,
    mask_ref,
    perm_ref,
    hist_ref,
    own_geo,
    geo,
    past,
    masked,
    moved_one,
    moved_two,
    perm_tiles,
    scaled_tiles,
    receiver,
    ends,
    own_columns,
    columns,
    pairs,
    feats,
    partial,
    counted,
    in_sems,
    send_sems,
    recv_sems,
    *lines,
):
    lines_one, lines_two = lines[: len(FIRST_GROUPS)], lines[len(FIRST_GROUPS) :]
    sems = [(send_sems.at[n], recv_sems.at[n]) for n in range(SEMS)]

    loads = [
        pltpu.make_async_copy(src, dst, in_sems.at[n])
        for n, (src, dst) in enumerate(
            (
                (frac_hbm, frac_ref),
                (pol_hbm, pol_ref),
                (occ_hbm, occ_ref),
                (hist_hbm, hist_ref),
                (mask_hbm, mask_ref),
                (perm_hbm, perm_ref),
            )
        )
    ]
    for load in loads:
        load.start()

    barrier = pltpu.get_barrier_semaphore()
    greeted = [neighbour(sizes, direction) for direction in DIRECTIONS]
    for axis in AXES:
        greeted += [{axis: away(sizes, axis, step)} for step in range(2, sizes[axis] - 1)]
    for device in greeted:
        pl.semaphore_signal(barrier, inc=1, device_id=device, device_id_type=MESH)

    lane = lax.broadcasted_iota(jnp.int32, (1, LANES), 1)
    sub = lax.broadcasted_iota(jnp.int32, (8, LANES), 0)
    lane16 = lax.broadcasted_iota(jnp.int32, (16, LANES), 1)
    sub16 = lax.broadcasted_iota(jnp.int32, (16, LANES), 0)

    loads[0].wait()
    loads[1].wait()
    for tile, (ry, rz) in enumerate(RECEIVERS):
        for which in range(2):
            for c in range(3):
                own_geo[tile, pl.ds(4 * which + c, 1)] = frac_ref[c, pl.ds(tile, 1), :]
            own_geo[tile, pl.ds(4 * which + 3, 1)] = pol_ref[pl.ds(tile, 1), :]
        geo[1, 1 + ry, 1 + rz] = own_geo[tile]

    def positions(slab, rows, sx, tile_y, tile_z):
        kind = lax.rem(rows, 4)
        shift = jnp.where(
            kind == 0,
            jnp.float32(sx - 1.5),
            jnp.where(kind == 1, (tile_y - 2).astype(F32), (tile_z - 2).astype(F32)),
        )
        at = (slab + shift) * CELL_EDGE
        return kind == 3, at, DAMP_ROOT * lax.rsqrt(slab)

    row32 = lax.broadcasted_iota(jnp.int32, (32, LANES), 0)
    last, at, root = positions(
        own_geo[...].reshape(32, LANES), row32, 1, 1 + row32 // 16, 1 + lax.rem(row32 // 8, 2)
    )
    receiver[...] = jnp.where(last, -root, at)
    own_columns[...] = jnp.transpose(
        jnp.concatenate([jnp.where(last, root, at), jnp.zeros((96, LANES), F32)], axis=0)
    )

    def pair_factors(cols, places, offset_of, sx, first):
        for at, sy, sz in places:
            source = [
                jnp.broadcast_to(cols[:, at + n : at + n + 1], (16, LANES)) for n in range(4)
            ]
            for tile, (ry, rz) in enumerate(RECEIVERS):
                ky, kz = sy - ry, sz - rz
                if not (0 <= ky <= 2 and 0 <= kz <= 2):
                    continue
                d = [source[n] - receiver[pl.ds(8 * tile + n, 1), :] for n in range(3)]
                damp = source[3] * receiver[pl.ds(8 * tile + 3, 1), :]
                offset = 9 * sx + 3 * ky + kz
                allowed = 3.0 * mask_ref[tile, offset].astype(F32)
                dist = d[0] * d[0] + d[1] * d[1] + d[2] * d[2] + SOFTENING
                root = lax.rsqrt(dist)
                inverse = root * root
                cube = root * inverse * allowed
                if offset_of == "own" and ky == 1 and kz == 1:
                    cube = jnp.where(sub16 + first != lane16, cube, 0.0)
                power = dist * dist * root * damp
                fade = jnp.exp2(power)
                three = 1.0 - fade
                five = three + (power * LN2) * fade
                for part, value in ((0, five * (inverse * cube)), (128, three * cube)):
                    high = value.astype(BF16)
                    low = (value - high.astype(F32)).astype(BF16)
                    rows = pl.ds(pl.multiple_of(first + part, 16), 16)
                    pairs[tile, offset, rows, pl.ds(0, 128)] = high
                    pairs[tile, offset, rows, pl.ds(128, 128)] = low

    loads[2].wait()
    loads[3].wait()
    filled = occ_ref[...].astype(F32)
    filled_rows = jnp.concatenate([filled] * 6, axis=0)
    for h in range(6):
        masked[h] = hist_ref[h] * filled_rows
    row = jnp.zeros((1, LANES), F32)
    for a in range(6):
        for b in range(a, 6):
            product = masked[a] * masked[b]
            folded = product[0:8] + product[8:16] + product[16:24]
            value = jnp.sum(jnp.sum(folded, axis=0, keepdims=True), axis=1, keepdims=True)
            row = jnp.where(lane == 6 * a + b, value, row)

    for tile, (ry, rz) in enumerate(RECEIVERS):
        own = (1, 1 + ry, 1 + rz)
        for h in range(5):
            past[own + (pl.ds(6 * h, 6),)] = masked[h + 1, pl.ds(tile, 6, stride=4), :]
        past[own + (pl.ds(30, 2),)] = jnp.zeros((2, LANES), F32)

    loads[4].wait()
    loads[5].wait()
    for tile in range(4):
        weight = jnp.broadcast_to(
            RELAXATION * occ_ref[pl.ds(tile, 1), :].astype(F32) * pol_ref[pl.ds(tile, 1), :],
            (8, LANES),
        )
        scaled_tiles[tile] = jnp.where(lax.rem(sub, 4) == 3, 0.0, weight)
        perm_tiles[tile] = jnp.zeros((8, LANES), F32)
        for which in range(2):
            perm_tiles[tile, pl.ds(4 * which, 3), :] = perm_ref[
                pl.ds(12 * which + tile, 3, stride=4), :
            ]

    own_places = [(8 * tile, 1 + ry, 1 + rz) for tile, (ry, rz) in enumerate(RECEIVERS)]
    all_places = [(8 * (4 * sy + sz), sy, sz) for sy in range(4) for sz in range(4)]
    rim_places = [(at, sy, sz) for at, sy, sz in all_places if sy in (0, 3) or sz in (0, 3)]

    def own_block(block, carry):
        first = pl.multiple_of(block * 16, 16)
        pair_factors(own_columns[pl.ds(first, 16), :], own_places, "own", 1, first)
        return carry

    lax.fori_loop(0, 8, own_block, 0)

    def clear(number, carry):
        sx, s = number // 16, lax.rem(number, 16)
        for piece in range(3):
            feats[sx, s, pl.ds(32 * piece, 16), pl.ds(128, 128)] = jnp.zeros((16, LANES), BF16)
        return carry

    lax.fori_loop(0, 48, clear, 0, unroll=4)

    def send_group(groups, number, bufs, first_sem, values):
        me, batch = group_batch(sizes, groups[number], bufs[number], sems[first_sem + number])
        bufs[number][me] = values
        batch.start()
        return batch

    def total(bufs, number, batch):
        batch.arrived()
        return jnp.sum(bufs[number][...], axis=0)

    pl.semaphore_wait(barrier, len(greeted))

    geo_batches = [halo_batch(sizes, geo, sems[n], n == 0) for n in range(2)]
    past_batches = [halo_batch(sizes, past, sems[2 + n], n == 0) for n in range(2)]
    line_a = send_group(FIRST_GROUPS, 0, lines_one, 8, row)
    for batch in geo_batches + past_batches:
        batch.start()

    row128 = lax.broadcasted_iota(jnp.int32, (LANES, LANES), 0)

    def place_slab(sx):
        last, at, root = positions(
            geo[sx].reshape(LANES, LANES), row128, sx, row128 // 32, lax.rem(row128 // 8, 4)
        )
        ends[sx] = jnp.where(last, 1.0, at)
        columns[sx] = jnp.transpose(jnp.where(last, root, at))

    geo_batches[0].arrived()
    place_slab(1)

    def rim_block(block, carry):
        first = pl.multiple_of(block * 16, 16)
        pair_factors(columns[1, pl.ds(first, 16), :], rim_places, "rim", 1, first)
        return carry

    lax.fori_loop(0, 8, rim_block, 0)

    row = total(lines_one, 0, line_a)
    line_b = send_group(FIRST_GROUPS, 1, lines_one, 8, row)

    geo_batches[1].arrived()
    place_slab(0)
    place_slab(2)

    def side_block(step, carry):
        sx = 2 * (step // 8)
        first = pl.multiple_of(lax.rem(step, 8) * 16, 16)
        pair_factors(columns[sx, pl.ds(first, 16), :], all_places, "side", sx, first)
        return carry

    lax.fori_loop(0, 11, side_block, 0)
    row = total(lines_one, 1, line_b)
    line_c = send_group(FIRST_GROUPS, 2, lines_one, 8, row)
    lax.fori_loop(11, 16, side_block, 0)
    row = total(lines_one, 2, line_c)

    def entry(a, b):
        return jnp.sum(
            jnp.where(lane == 6 * min(a, b) + max(a, b), row, 0.0), axis=1, keepdims=True
        )

    gram = {(a, b): entry(a, b) for a in range(6) for b in range(a, 6) if a < 5}
    trace = gram[0, 0] + gram[1, 1] + gram[2, 2] + gram[3, 3] + gram[4, 4]
    ridge = 0.001 * trace / 5.0 + 1.0
    low = {}
    scale = []
    half = []
    for a in range(5):
        pivot = gram[a, a] + ridge
        for c in range(a):
            pivot = pivot - low[a, c] * low[a, c]
        scale.append(lax.rsqrt(pivot))
        for b in range(a + 1, 5):
            value = gram[a, b]
            for c in range(a):
                value = value - low[a, c] * low[b, c]
            low[b, a] = value * scale[a]
        value = gram[a, 5]
        for c in range(a):
            value = value - low[a, c] * half[c]
        half.append(value * scale[a])
    coeffs = [None] * 5
    for a in reversed(range(5)):
        value = half[a]
        for b in range(a + 1, 5):
            value = value - low[b, a] * coeffs[b]
        coeffs[a] = value * scale[a]
    coeffs = [jnp.broadcast_to(value, (8, LANES))[0:6] for value in coeffs]

    past_batches[0].arrived()
    past_batches[1].arrived()

    first_set = sub < 4
    flat = jnp.zeros((8, LANES), F32)

    def write_feats(sx, s, tile_ref):
        whole = tile_ref[...]
        near = ends[sx, pl.ds(8 * s, 8), :]
        multipliers = []
        along = None
        for b in range(3):
            both = jnp.where(first_set, whole[b : b + 1], whole[4 + b : 5 + b])
            multipliers.append(both)
            term = near[b : b + 1] * both
            along = term if along is None else along + term
        multipliers.append(along)
        parts = [near * value for value in multipliers]
        for half_at in range(2):
            value = jnp.concatenate(parts[2 * half_at : 2 * half_at + 2], axis=0)
            for piece in range(3):
                kept = value.astype(BF16)
                feats[sx, s, pl.ds(32 * piece + 16 * half_at, 16), pl.ds(0, 128)] = kept
                value = value - kept.astype(F32)
        value = jnp.concatenate([flat, whole * (-1.0 / 3.0)], axis=0)
        for piece in range(3):
            kept = value.astype(BF16)
            feats[sx, s, pl.ds(32 * piece + 16, 16), pl.ds(128, 128)] = kept
            value = value - kept.astype(F32)

    def predict(sx, carry):
        for s in range(16):
            sy, sz = s // 4, s % 4
            value = None
            for h in range(5):
                term = coeffs[h] * past[sx, sy, sz, pl.ds(6 * h, 6), :]
                value = term if value is None else value + term
            moved_one[sx, sy, sz] = flat
            moved_one[sx, sy, sz, pl.ds(0, 3), :] = value[0:3]
            moved_one[sx, sy, sz, pl.ds(4, 3), :] = value[3:6]
        for s in range(16):
            write_feats(sx, s, moved_one.at[sx, s // 4, s % 4])
        return carry

    lax.fori_loop(0, 3, predict, 0)

    def dot_part(tile, sources):
        ry, rz = RECEIVERS[tile]
        lhs = jnp.concatenate([feats[sx, 4 * sy + sz] for sx, sy, sz in sources], axis=1)
        rhs = jnp.concatenate(
            [pairs[tile, 9 * sx + 3 * (sy - ry) + sz - rz] for sx, sy, sz in sources], axis=0
        )
        return jnp.dot(lhs, rhs, preferred_element_type=F32)

    def sources_of(tile, kinds=None):
        ry, rz = RECEIVERS[tile]
        return [
            (sx, ry + ky, rz + kz)
            for sx in range(3)
            for ky in range(3)
            for kz in range(3)
            if kinds is None or ((ry + ky + 1) % 2, (rz + kz + 1) % 2) == kinds
        ]

    def relaxed(tile, before, summed):
        both = summed[:, 0:128] + summed[:, 128:256]
        out = both[0:32] + both[32:64] + both[64:96]
        ry, rz = RECEIVERS[tile]
        here = ends[1, pl.ds(8 * (4 * (ry + 1) + rz + 1), 8), :]
        value = out[24:32]
        for b in range(3):
            value = value - here[b : b + 1] * out[8 * b : 8 * b + 8]
        shared = jnp.where(first_set, value[3:4], value[7:8])
        field = value - here * shared
        return (1.0 - RELAXATION) * before + scaled_tiles[tile] * (perm_tiles[tile] + field)

    tile_batches = []
    for tile, (ry, rz) in enumerate(RECEIVERS):
        before = moved_one[1, 1 + ry, 1 + rz]
        moved_two[1, 1 + ry, 1 + rz] = relaxed(tile, before, dot_part(tile, sources_of(tile)))
        tile_batches.append(tile_batch(sizes, moved_two, sems[4 + tile], tile, counted))
        tile_batches[-1].start()

    for batch in geo_batches + past_batches + [line_a, line_b, line_c]:
        batch.sent()

    changed = flat
    size = flat
    for kind, kinds in enumerate(RECEIVERS):
        tile_batches[kind].arrived()
        tiles = [
            (sy, sz)
            for sy in range(4)
            for sz in range(4)
            if ((sy + 1) % 2, (sz + 1) % 2) == kinds
        ]
        for sx in range(3):
            for sy, sz in tiles:
                write_feats(sx, 4 * sy + sz, moved_two.at[sx, sy, sz])
        for tile, (ry, rz) in enumerate(RECEIVERS):
            summed = dot_part(tile, sources_of(tile, kinds))
            if kind > 0:
                summed = summed + partial[tile]
            if kind < 3:
                partial[tile] = summed
                continue
            before = moved_two[1, 1 + ry, 1 + rz]
            after = relaxed(tile, before, summed)
            out_ref[pl.ds(tile, 3, stride=4), :] = after[0:3]
            out_ref[pl.ds(12 + tile, 3, stride=4), :] = after[4:7]
            update = after - before
            changed = changed + update * update
            size = size + after * after

    def whole_sum(value):
        return jnp.sum(jnp.sum(value, axis=0, keepdims=True), axis=1, keepdims=True)

    row = jnp.where(lane == 0, whole_sum(changed), jnp.where(lane == 1, whole_sum(size), 0.0))
    ending = []
    for number in range(len(LAST_GROUPS)):
        ending.append(send_group(LAST_GROUPS, number, lines_two, 8 + len(FIRST_GROUPS), row))
        if number == 0:
            for batch in tile_batches:
                batch.sent()
        row = total(lines_two, number, ending[-1])
    top = jnp.sum(jnp.where(lane == 0, row, 0.0), axis=1, keepdims=True)
    bottom = jnp.sum(jnp.where(lane == 1, row, 0.0), axis=1, keepdims=True)
    change_ref[...] = jnp.broadcast_to(jnp.sqrt(top / (bottom + 1.0)), (1, LANES))

    for batch in ending:
        batch.sent()


def on_device(sizes, fractions, polarizability, occupancy, pair_mask, perm_field, history):
    vmem = pl.BlockSpec(memory_space=pltpu.VMEM)
    hbm = pl.BlockSpec(memory_space=pltpu.HBM)
    dma = pltpu.SemaphoreType.DMA
    line_bufs = [
        pltpu.VMEM((math.prod(sizes[axis] for axis in axes), 1, LANES), F32)
        for axes in FIRST_GROUPS + LAST_GROUPS
    ]
    scratch = [
        pltpu.VMEM((3, 4, LANES), F32),
        pltpu.VMEM((4, LANES), F32),
        pltpu.VMEM((4, LANES), jnp.int32),
        pltpu.SMEM((4, 27), jnp.int32),
        pltpu.VMEM((24, LANES), F32),
        pltpu.VMEM((6, 24, LANES), F32),
        pltpu.VMEM((4, 8, LANES), F32),
        pltpu.VMEM((3, 4, 4, 8, LANES), F32),
        pltpu.VMEM((3, 4, 4, 32, LANES), F32),
        pltpu.VMEM((6, 24, LANES), F32),
        pltpu.VMEM((3, 4, 4, 8, LANES), F32),
        pltpu.VMEM((3, 4, 4, 8, LANES), F32),
        pltpu.VMEM((4, 8, LANES), F32),
        pltpu.VMEM((4, 8, LANES), F32),
        pltpu.VMEM((32, LANES), F32),
        pltpu.VMEM((3, LANES, LANES), F32),
        pltpu.VMEM((LANES, LANES), F32),
        pltpu.VMEM((3, LANES, LANES), F32),
        pltpu.VMEM((4, 27, 256, 256), BF16),
        pltpu.VMEM((3, 16, 96, 256), BF16),
        pltpu.VMEM((4, 96, 256), F32),
        pltpu.VMEM((11, 8, LANES), F32),
        dma((6,)),
        dma((SEMS,)),
        dma((SEMS,)),
    ]
    induced, change = pl.pallas_call(
        lambda *refs: kernel(sizes, *refs),
        out_shape=(
            jax.ShapeDtypeStruct((24, LANES), F32),
            jax.ShapeDtypeStruct((1, LANES), F32),
        ),
        in_specs=[hbm] * 6,
        out_specs=(vmem, vmem),
        scratch_shapes=scratch + line_bufs,
        compiler_params=pltpu.CompilerParams(
            collective_id=0, has_side_effects=True, vmem_limit_bytes=VMEM_BYTES
        ),
    )(
        fractions.reshape(3, 4, LANES),
        polarizability.reshape(4, LANES),
        occupancy.reshape(4, LANES),
        pair_mask.reshape(4, 27),
        perm_field.reshape(24, LANES),
        history.reshape(6, 24, LANES),
    )
    return induced.reshape(6, 1, 2, 2, LANES), change[0, 0]


def solution(mesh):
    sizes = {axis: mesh.shape[axis] for axis in AXES}
    placed = (
        P(None, "gx", "gy", "gz", None),
        P("gx", "gy", "gz", None),
        P("gx", "gy", "gz", None),
        P("gx", "gy", "gz", None),
        P(None, "gx", "gy", "gz", None),
        P(None, None, "gx", "gy", "gz", None),
    )
    return jax.shard_map(
        lambda *args: on_device(sizes, *args),
        mesh=mesh,
        in_specs=placed,
        out_specs=(P(None, "gx", "gy", "gz", None), P()),
        check_vma=False,
    )
```

```python
import math

import jax
import jax.numpy as jnp
from jax import lax
from jax.experimental import pallas as pl
from jax.experimental.pallas import tpu as pltpu
from jax.sharding import PartitionSpec as P

AXES = ("gx", "gy", "gz")
FIRST_GROUPS = (("gy",), ("gz",), ("gx",))
LAST_GROUPS = (("gx",), ("gy", "gz"))
MESH = pl.DeviceIdType.MESH
F32 = jnp.float32
BF16 = jnp.bfloat16
LANES = 128
DIRECTIONS = [
    (dx, dy, dz)
    for dx in (-1, 0, 1)
    for dy in (-1, 0, 1)
    for dz in (-1, 0, 1)
    if (dx, dy, dz) != (0, 0, 0)
]
CELL_EDGE = 10.0
SOFTENING = 0.3
THOLE_DAMP = 0.39
RELAXATION = 0.7
LN2 = math.log(2.0)
DAMP_ROOT = math.sqrt(THOLE_DAMP / LN2)
RECEIVERS = [(ry, rz) for ry in (0, 1) for rz in (0, 1)]


SEMS = 8 + len(FIRST_GROUPS) + len(LAST_GROUPS)
VMEM_BYTES = 40 * 1024 * 1024


def away(sizes, axis, step):
    return lax.rem(lax.axis_index(axis) + (step + sizes[axis]), sizes[axis])


def neighbour(sizes, direction):
    return {axis: away(sizes, axis, step) for axis, step in zip(AXES, direction) if step != 0}


def sent_part(step):
    return {0: pl.ds(1, 2), 1: pl.ds(2, 1), -1: pl.ds(1, 1)}[step]


def landing_part(step):
    return {0: pl.ds(1, 2), 1: pl.ds(0, 1), -1: pl.ds(3, 1)}[step]


def remote(src, dst, sems, device):
    return pltpu.make_async_remote_copy(
        src_ref=src,
        dst_ref=dst,
        send_sem=sems[0],
        recv_sem=sems[1],
        device_id=device,
        device_id_type=MESH,
    )


class Batch:
    def __init__(self, copies, counted, sems, device):
        self.copies = copies
        self.whole = remote(counted, counted, sems, device)

    def start(self):
        for copy in self.copies:
            copy.start()

    def arrived(self):
        self.whole.wait_recv()

    def sent(self):
        self.whole.wait_send()


def halo_batch(sizes, buf, sems, same_slab):
    copies = []
    for direction in DIRECTIONS:
        dx, dy, dz = direction
        if (dx == 0) != same_slab:
            continue
        copies.append(
            remote(
                buf.at[pl.ds(1, 1), sent_part(dy), sent_part(dz)],
                buf.at[pl.ds(1 - dx, 1), landing_part(dy), landing_part(dz)],
                sems,
                neighbour(sizes, direction),
            )
        )
    counted = buf.at[1, pl.ds(0, 3)] if same_slab else buf.at[pl.ds(0, 2)]
    return Batch(copies, counted, sems, neighbour(sizes, (0, 0, 1)))


def tile_batch(sizes, buf, sems, tile, counted):
    ry, rz = RECEIVERS[tile]
    mine = buf.at[1, 1 + ry, 1 + rz]
    copies = []
    for dx in (-1, 0, 1):
        for dy, at_y in ((0, 1 + ry), (2 * ry - 1, 3 - 3 * ry)):
            for dz, at_z in ((0, 1 + rz), (2 * rz - 1, 3 - 3 * rz)):
                if (dx, dy, dz) != (0, 0, 0):
                    copies.append(
                        remote(
                            mine,
                            buf.at[1 - dx, at_y, at_z],
                            sems,
                            neighbour(sizes, (dx, dy, dz)),
                        )
                    )
    return Batch(copies, counted, sems, neighbour(sizes, (0, 0, 1)))


def group_steps(sizes, axes):
    steps = [()]
    for axis in axes:
        steps = [step + (n,) for step in steps for n in range(sizes[axis])]
    far = lambda step: sum(min(n, sizes[axis] - n) for n, axis in zip(step, axes))
    return sorted([step for step in steps if any(step)], key=far, reverse=True)


def group_batch(sizes, axes, buf, sems):
    me = 0
    for axis in axes:
        me = me * sizes[axis] + lax.axis_index(axis)
    copies = []
    for step in group_steps(sizes, axes):
        device = {axis: away(sizes, axis, n) for axis, n in zip(axes, step) if n != 0}
        copies.append(remote(buf.at[me], buf.at[me], sems, device))
    counted = buf.at[pl.ds(0, len(copies))]
    return me, Batch(copies, counted, sems, {axes[0]: away(sizes, axes[0], 1)})


def kernel(
    sizes,
    frac_hbm,
    pol_hbm,
    occ_hbm,
    mask_hbm,
    perm_hbm,
    hist_hbm,
    out_ref,
    change_ref,
    frac_ref,
    pol_ref,
    occ_ref,
    mask_ref,
    perm_ref,
    hist_ref,
    own_geo,
    geo,
    past,
    masked,
    moved_one,
    moved_two,
    perm_tiles,
    scaled_tiles,
    receiver,
    ends,
    own_columns,
    columns,
    pairs,
    feats,
    partial,
    counted,
    in_sems,
    send_sems,
    recv_sems,
    *lines,
):
    lines_one, lines_two = lines[: len(FIRST_GROUPS)], lines[len(FIRST_GROUPS) :]
    sems = [(send_sems.at[n], recv_sems.at[n]) for n in range(SEMS)]

    loads = [
        pltpu.make_async_copy(src, dst, in_sems.at[n])
        for n, (src, dst) in enumerate(
            (
                (frac_hbm, frac_ref),
                (pol_hbm, pol_ref),
                (occ_hbm, occ_ref),
                (hist_hbm, hist_ref),
                (mask_hbm, mask_ref),
                (perm_hbm, perm_ref),
            )
        )
    ]
    for load in loads:
        load.start()

    barrier = pltpu.get_barrier_semaphore()
    greeted = []
    for axis in ("gz", "gx", "gy"):
        greeted += [
            {axis: away(sizes, axis, step)}
            for (step,) in group_steps(sizes, (axis,))
            if 2 <= step <= sizes[axis] - 2
        ]
    greeted += [neighbour(sizes, direction) for direction in DIRECTIONS]
    for device in greeted:
        pl.semaphore_signal(barrier, inc=1, device_id=device, device_id_type=MESH)

    lane = lax.broadcasted_iota(jnp.int32, (1, LANES), 1)
    sub = lax.broadcasted_iota(jnp.int32, (8, LANES), 0)
    lane16 = lax.broadcasted_iota(jnp.int32, (16, LANES), 1)
    sub16 = lax.broadcasted_iota(jnp.int32, (16, LANES), 0)

    loads[0].wait()
    loads[1].wait()
    for tile, (ry, rz) in enumerate(RECEIVERS):
        for which in range(2):
            for c in range(3):
                own_geo[tile, pl.ds(4 * which + c, 1)] = frac_ref[c, pl.ds(tile, 1), :]
            own_geo[tile, pl.ds(4 * which + 3, 1)] = pol_ref[pl.ds(tile, 1), :]
        geo[1, 1 + ry, 1 + rz] = own_geo[tile]

    def positions(slab, rows, sx, tile_y, tile_z):
        kind = lax.rem(rows, 4)
        shift = jnp.where(
            kind == 0,
            jnp.float32(sx - 1.5),
            jnp.where(kind == 1, (tile_y - 2).astype(F32), (tile_z - 2).astype(F32)),
        )
        at = (slab + shift) * CELL_EDGE
        return kind == 3, at, DAMP_ROOT * lax.rsqrt(slab)

    row32 = lax.broadcasted_iota(jnp.int32, (32, LANES), 0)
    last, at, root = positions(
        own_geo[...].reshape(32, LANES), row32, 1, 1 + row32 // 16, 1 + lax.rem(row32 // 8, 2)
    )
    receiver[...] = jnp.where(last, -root, at)
    own_columns[...] = jnp.transpose(
        jnp.concatenate([jnp.where(last, root, at), jnp.zeros((96, LANES), F32)], axis=0)
    )

    def pair_factors(cols, places, offset_of, sx, first):
        for at, sy, sz in places:
            source = [
                jnp.broadcast_to(cols[:, at + n : at + n + 1], (16, LANES)) for n in range(4)
            ]
            for tile, (ry, rz) in enumerate(RECEIVERS):
                ky, kz = sy - ry, sz - rz
                if not (0 <= ky <= 2 and 0 <= kz <= 2):
                    continue
                d = [source[n] - receiver[pl.ds(8 * tile + n, 1), :] for n in range(3)]
                damp = source[3] * receiver[pl.ds(8 * tile + 3, 1), :]
                offset = 9 * sx + 3 * ky + kz
                allowed = 3.0 * mask_ref[tile, offset].astype(F32)
                dist = d[0] * d[0] + d[1] * d[1] + d[2] * d[2] + SOFTENING
                root = lax.rsqrt(dist)
                inverse = root * root
                cube = root * inverse * allowed
                if offset_of == "own" and ky == 1 and kz == 1:
                    cube = jnp.where(sub16 + first != lane16, cube, 0.0)
                power = dist * dist * root * damp
                fade = jnp.exp2(power)
                three = 1.0 - fade
                five = three + (power * LN2) * fade
                for part, value in ((0, five * (inverse * cube)), (128, three * cube)):
                    high = value.astype(BF16)
                    low = (value - high.astype(F32)).astype(BF16)
                    rows = pl.ds(pl.multiple_of(first + part, 16), 16)
                    pairs[tile, offset, rows, pl.ds(0, 128)] = high
                    pairs[tile, offset, rows, pl.ds(128, 128)] = low

    loads[2].wait()
    loads[3].wait()
    filled = occ_ref[...].astype(F32)
    filled_rows = jnp.concatenate([filled] * 6, axis=0)
    for h in range(6):
        masked[h] = hist_ref[h] * filled_rows
    row = jnp.zeros((1, LANES), F32)
    for a in range(6):
        for b in range(a, 6):
            product = masked[a] * masked[b]
            folded = product[0:8] + product[8:16] + product[16:24]
            value = jnp.sum(jnp.sum(folded, axis=0, keepdims=True), axis=1, keepdims=True)
            row = jnp.where(lane == 6 * a + b, value, row)

    for tile, (ry, rz) in enumerate(RECEIVERS):
        own = (1, 1 + ry, 1 + rz)
        for h in range(5):
            past[own + (pl.ds(6 * h, 6),)] = masked[h + 1, pl.ds(tile, 6, stride=4), :]
        past[own + (pl.ds(30, 2),)] = jnp.zeros((2, LANES), F32)

    loads[4].wait()
    loads[5].wait()
    for tile in range(4):
        weight = jnp.broadcast_to(
            RELAXATION * occ_ref[pl.ds(tile, 1), :].astype(F32) * pol_ref[pl.ds(tile, 1), :],
            (8, LANES),
        )
        scaled_tiles[tile] = jnp.where(lax.rem(sub, 4) == 3, 0.0, weight)
        perm_tiles[tile] = jnp.zeros((8, LANES), F32)
        for which in range(2):
            perm_tiles[tile, pl.ds(4 * which, 3), :] = perm_ref[
                pl.ds(12 * which + tile, 3, stride=4), :
            ]

    own_places = [(8 * tile, 1 + ry, 1 + rz) for tile, (ry, rz) in enumerate(RECEIVERS)]
    all_places = [(8 * (4 * sy + sz), sy, sz) for sy in range(4) for sz in range(4)]
    rim_places = [(at, sy, sz) for at, sy, sz in all_places if sy in (0, 3) or sz in (0, 3)]

    def own_block(block, carry):
        first = pl.multiple_of(block * 16, 16)
        pair_factors(own_columns[pl.ds(first, 16), :], own_places, "own", 1, first)
        return carry

    lax.fori_loop(0, 8, own_block, 0)

    def clear(number, carry):
        sx, s = number // 16, lax.rem(number, 16)
        for piece in range(3):
            feats[sx, s, pl.ds(32 * piece, 16), pl.ds(128, 128)] = jnp.zeros((16, LANES), BF16)
        return carry

    lax.fori_loop(0, 48, clear, 0, unroll=4)

    def send_group(groups, number, bufs, first_sem, values):
        me, batch = group_batch(sizes, groups[number], bufs[number], sems[first_sem + number])
        bufs[number][me] = values
        batch.start()
        return batch

    def total(bufs, number, batch):
        batch.arrived()
        return jnp.sum(bufs[number][...], axis=0)

    pl.semaphore_wait(barrier, len(greeted))

    geo_batches = [halo_batch(sizes, geo, sems[n], n == 0) for n in range(2)]
    past_batches = [halo_batch(sizes, past, sems[2 + n], n == 0) for n in range(2)]
    line_a = send_group(FIRST_GROUPS, 0, lines_one, 8, row)
    for batch in geo_batches + past_batches:
        batch.start()

    row = total(lines_one, 0, line_a)
    line_b = send_group(FIRST_GROUPS, 1, lines_one, 8, row)

    row128 = lax.broadcasted_iota(jnp.int32, (LANES, LANES), 0)

    def place_slab(sx):
        last, at, root = positions(
            geo[sx].reshape(LANES, LANES), row128, sx, row128 // 32, lax.rem(row128 // 8, 4)
        )
        ends[sx] = jnp.where(last, 1.0, at)
        columns[sx] = jnp.transpose(jnp.where(last, root, at))

    geo_batches[0].arrived()
    place_slab(1)

    def rim_block(block, carry):
        first = pl.multiple_of(block * 16, 16)
        pair_factors(columns[1, pl.ds(first, 16), :], rim_places, "rim", 1, first)
        return carry

    lax.fori_loop(0, 8, rim_block, 0)

    geo_batches[1].arrived()
    place_slab(0)
    place_slab(2)

    def side_block(step, carry):
        sx = 2 * (step // 8)
        first = pl.multiple_of(lax.rem(step, 8) * 16, 16)
        pair_factors(columns[sx, pl.ds(first, 16), :], all_places, "side", sx, first)
        return carry

    lax.fori_loop(0, 4, side_block, 0)
    row = total(lines_one, 1, line_b)
    line_c = send_group(FIRST_GROUPS, 2, lines_one, 8, row)
    lax.fori_loop(4, 16, side_block, 0)
    row = total(lines_one, 2, line_c)

    def entry(a, b):
        return jnp.sum(
            jnp.where(lane == 6 * min(a, b) + max(a, b), row, 0.0), axis=1, keepdims=True
        )

    gram = {(a, b): entry(a, b) for a in range(6) for b in range(a, 6) if a < 5}
    trace = gram[0, 0] + gram[1, 1] + gram[2, 2] + gram[3, 3] + gram[4, 4]
    ridge = 0.001 * trace / 5.0 + 1.0
    low = {}
    scale = []
    half = []
    for a in range(5):
        pivot = gram[a, a] + ridge
        for c in range(a):
            pivot = pivot - low[a, c] * low[a, c]
        scale.append(lax.rsqrt(pivot))
        for b in range(a + 1, 5):
            value = gram[a, b]
            for c in range(a):
                value = value - low[a, c] * low[b, c]
            low[b, a] = value * scale[a]
        value = gram[a, 5]
        for c in range(a):
            value = value - low[a, c] * half[c]
        half.append(value * scale[a])
    coeffs = [None] * 5
    for a in reversed(range(5)):
        value = half[a]
        for b in range(a + 1, 5):
            value = value - low[b, a] * coeffs[b]
        coeffs[a] = value * scale[a]
    coeffs = [jnp.broadcast_to(value, (8, LANES))[0:6] for value in coeffs]

    past_batches[0].arrived()
    past_batches[1].arrived()

    first_set = sub < 4
    flat = jnp.zeros((8, LANES), F32)

    def write_feats(sx, s, tile_ref):
        whole = tile_ref[...]
        near = ends[sx, pl.ds(8 * s, 8), :]
        multipliers = []
        along = None
        for b in range(3):
            both = jnp.where(first_set, whole[b : b + 1], whole[4 + b : 5 + b])
            multipliers.append(both)
            term = near[b : b + 1] * both
            along = term if along is None else along + term
        multipliers.append(along)
        parts = [near * value for value in multipliers]
        for half_at in range(2):
            value = jnp.concatenate(parts[2 * half_at : 2 * half_at + 2], axis=0)
            for piece in range(3):
                kept = value.astype(BF16)
                feats[sx, s, pl.ds(32 * piece + 16 * half_at, 16), pl.ds(0, 128)] = kept
                value = value - kept.astype(F32)
        value = jnp.concatenate([flat, whole * (-1.0 / 3.0)], axis=0)
        for piece in range(3):
            kept = value.astype(BF16)
            feats[sx, s, pl.ds(32 * piece + 16, 16), pl.ds(128, 128)] = kept
            value = value - kept.astype(F32)

    def predict(sx, carry):
        for s in range(16):
            sy, sz = s // 4, s % 4
            value = None
            for h in range(5):
                term = coeffs[h] * past[sx, sy, sz, pl.ds(6 * h, 6), :]
                value = term if value is None else value + term
            moved_one[sx, sy, sz] = flat
            moved_one[sx, sy, sz, pl.ds(0, 3), :] = value[0:3]
            moved_one[sx, sy, sz, pl.ds(4, 3), :] = value[3:6]
        for s in range(16):
            write_feats(sx, s, moved_one.at[sx, s // 4, s % 4])
        return carry

    lax.fori_loop(0, 3, predict, 0)

    def dot_part(tile, sources):
        if len(sources) > 6:
            middle = len(sources) // 2
            return dot_piece(tile, sources[:middle]) + dot_piece(tile, sources[middle:])
        return dot_piece(tile, sources)

    def dot_piece(tile, sources):
        ry, rz = RECEIVERS[tile]
        lhs = jnp.concatenate([feats[sx, 4 * sy + sz] for sx, sy, sz in sources], axis=1)
        rhs = jnp.concatenate(
            [pairs[tile, 9 * sx + 3 * (sy - ry) + sz - rz] for sx, sy, sz in sources], axis=0
        )
        return jnp.dot(lhs, rhs, preferred_element_type=F32)

    def sources_of(tile, kinds=None):
        ry, rz = RECEIVERS[tile]
        return [
            (sx, ry + ky, rz + kz)
            for sx in range(3)
            for ky in range(3)
            for kz in range(3)
            if kinds is None or ((ry + ky + 1) % 2, (rz + kz + 1) % 2) == kinds
        ]

    def relaxed(tile, before, summed):
        both = summed[:, 0:128] + summed[:, 128:256]
        out = both[0:32] + both[32:64] + both[64:96]
        ry, rz = RECEIVERS[tile]
        here = ends[1, pl.ds(8 * (4 * (ry + 1) + rz + 1), 8), :]
        value = out[24:32]
        for b in range(3):
            value = value - here[b : b + 1] * out[8 * b : 8 * b + 8]
        shared = jnp.where(first_set, value[3:4], value[7:8])
        field = value - here * shared
        return (1.0 - RELAXATION) * before + scaled_tiles[tile] * (perm_tiles[tile] + field)

    tile_batches = []
    summed = dot_part(0, sources_of(0))
    for tile, (ry, rz) in enumerate(RECEIVERS):
        now = summed
        if tile < 3:
            summed = dot_part(tile + 1, sources_of(tile + 1))
        before = moved_one[1, 1 + ry, 1 + rz]
        moved_two[1, 1 + ry, 1 + rz] = relaxed(tile, before, now)
        tile_batches.append(tile_batch(sizes, moved_two, sems[4 + tile], tile, counted))
        tile_batches[-1].start()

    for batch in geo_batches + past_batches + [line_a, line_b, line_c]:
        batch.sent()

    changed = flat
    size = flat
    for kind, kinds in enumerate(RECEIVERS):
        tile_batches[kind].arrived()
        tiles = [
            (sy, sz)
            for sy in range(4)
            for sz in range(4)
            if ((sy + 1) % 2, (sz + 1) % 2) == kinds
        ]
        for sx in range(3):
            for sy, sz in tiles:
                write_feats(sx, 4 * sy + sz, moved_two.at[sx, sy, sz])
        for tile, (ry, rz) in enumerate(RECEIVERS):
            summed = dot_part(tile, sources_of(tile, kinds))
            if kind > 0:
                summed = summed + partial[tile]
            if kind < 3:
                partial[tile] = summed
                continue
            before = moved_two[1, 1 + ry, 1 + rz]
            after = relaxed(tile, before, summed)
            out_ref[pl.ds(tile, 3, stride=4), :] = after[0:3]
            out_ref[pl.ds(12 + tile, 3, stride=4), :] = after[4:7]
            update = after - before
            changed = changed + update * update
            size = size + after * after

    def whole_sum(value):
        return jnp.sum(jnp.sum(value, axis=0, keepdims=True), axis=1, keepdims=True)

    row = jnp.where(lane == 0, whole_sum(changed), jnp.where(lane == 1, whole_sum(size), 0.0))
    ending = []
    for number in range(len(LAST_GROUPS)):
        ending.append(send_group(LAST_GROUPS, number, lines_two, 8 + len(FIRST_GROUPS), row))
        if number == 0:
            for batch in tile_batches:
                batch.sent()
        row = total(lines_two, number, ending[-1])
    top = jnp.sum(jnp.where(lane == 0, row, 0.0), axis=1, keepdims=True)
    bottom = jnp.sum(jnp.where(lane == 1, row, 0.0), axis=1, keepdims=True)
    change_ref[...] = jnp.broadcast_to(jnp.sqrt(top / (bottom + 1.0)), (1, LANES))

    for batch in ending:
        batch.sent()


def in_hbm(array):
    return pltpu.with_memory_space_constraint(array, pltpu.HBM)


def on_device(sizes, fractions, polarizability, occupancy, pair_mask, perm_field, history):
    vmem = pl.BlockSpec(memory_space=pltpu.VMEM)
    hbm = pl.BlockSpec(memory_space=pltpu.HBM)
    dma = pltpu.SemaphoreType.DMA
    line_bufs = [
        pltpu.VMEM((math.prod(sizes[axis] for axis in axes), 1, LANES), F32)
        for axes in FIRST_GROUPS + LAST_GROUPS
    ]
    scratch = [
        pltpu.VMEM((3, 4, LANES), F32),
        pltpu.VMEM((4, LANES), F32),
        pltpu.VMEM((4, LANES), jnp.int32),
        pltpu.SMEM((4, 27), jnp.int32),
        pltpu.VMEM((24, LANES), F32),
        pltpu.VMEM((6, 24, LANES), F32),
        pltpu.VMEM((4, 8, LANES), F32),
        pltpu.VMEM((3, 4, 4, 8, LANES), F32),
        pltpu.VMEM((3, 4, 4, 32, LANES), F32),
        pltpu.VMEM((6, 24, LANES), F32),
        pltpu.VMEM((3, 4, 4, 8, LANES), F32),
        pltpu.VMEM((3, 4, 4, 8, LANES), F32),
        pltpu.VMEM((4, 8, LANES), F32),
        pltpu.VMEM((4, 8, LANES), F32),
        pltpu.VMEM((32, LANES), F32),
        pltpu.VMEM((3, LANES, LANES), F32),
        pltpu.VMEM((LANES, LANES), F32),
        pltpu.VMEM((3, LANES, LANES), F32),
        pltpu.VMEM((4, 27, 256, 256), BF16),
        pltpu.VMEM((3, 16, 96, 256), BF16),
        pltpu.VMEM((4, 96, 256), F32),
        pltpu.VMEM((11, 8, LANES), F32),
        dma((6,)),
        dma((SEMS,)),
        dma((SEMS,)),
    ]
    induced, change = pl.pallas_call(
        lambda *refs: kernel(sizes, *refs),
        out_shape=(
            jax.ShapeDtypeStruct((24, LANES), F32),
            jax.ShapeDtypeStruct((1, LANES), F32),
        ),
        in_specs=[hbm] * 6,
        out_specs=(vmem, vmem),
        scratch_shapes=scratch + line_bufs,
        compiler_params=pltpu.CompilerParams(
            collective_id=0, has_side_effects=True, vmem_limit_bytes=VMEM_BYTES
        ),
    )(
        in_hbm(fractions.reshape(3, 4, LANES)),
        in_hbm(polarizability.reshape(4, LANES)),
        in_hbm(occupancy.reshape(4, LANES)),
        in_hbm(pair_mask.reshape(4, 27)),
        in_hbm(perm_field.reshape(24, LANES)),
        in_hbm(history.reshape(6, 24, LANES)),
    )
    return induced.reshape(6, 1, 2, 2, LANES), change[0, 0]


def solution(mesh):
    sizes = {axis: mesh.shape[axis] for axis in AXES}
    placed = (
        P(None, "gx", "gy", "gz", None),
        P("gx", "gy", "gz", None),
        P("gx", "gy", "gz", None),
        P("gx", "gy", "gz", None),
        P(None, "gx", "gy", "gz", None),
        P(None, None, "gx", "gy", "gz", None),
    )
    return jax.shard_map(
        lambda *args: on_device(sizes, *args),
        mesh=mesh,
        in_specs=placed,
        out_specs=(P(None, "gx", "gy", "gz", None), P()),
        check_vma=False,
    )
```

```python
import math

import jax
import jax.numpy as jnp
from jax import lax
from jax.experimental import pallas as pl
from jax.experimental.pallas import tpu as pltpu
from jax.sharding import PartitionSpec as P

AXES = ("gx", "gy", "gz")
FIRST_GROUPS = (("gy",), ("gx",), ("gz",))
LAST_GROUPS = (("gx",), ("gy", "gz"))
MESH = pl.DeviceIdType.MESH
F32 = jnp.float32
BF16 = jnp.bfloat16
LANES = 128
DIRECTIONS = [
    (dx, dy, dz)
    for dx in (-1, 0, 1)
    for dy in (-1, 0, 1)
    for dz in (-1, 0, 1)
    if (dx, dy, dz) != (0, 0, 0)
]
CELL_EDGE = 10.0
SOFTENING = 0.3
THOLE_DAMP = 0.39
RELAXATION = 0.7
LN2 = math.log(2.0)
DAMP_ROOT = math.sqrt(THOLE_DAMP / LN2)
RECEIVERS = [(ry, rz) for ry in (0, 1) for rz in (0, 1)]


SEMS = 8 + len(FIRST_GROUPS) + len(LAST_GROUPS)
VMEM_BYTES = 40 * 1024 * 1024


def away(sizes, axis, step):
    return lax.rem(lax.axis_index(axis) + (step + sizes[axis]), sizes[axis])


def neighbour(sizes, direction):
    return {axis: away(sizes, axis, step) for axis, step in zip(AXES, direction) if step != 0}


def sent_part(step):
    return {0: pl.ds(1, 2), 1: pl.ds(2, 1), -1: pl.ds(1, 1)}[step]


def landing_part(step):
    return {0: pl.ds(1, 2), 1: pl.ds(0, 1), -1: pl.ds(3, 1)}[step]


def remote(src, dst, sems, device):
    return pltpu.make_async_remote_copy(
        src_ref=src,
        dst_ref=dst,
        send_sem=sems[0],
        recv_sem=sems[1],
        device_id=device,
        device_id_type=MESH,
    )


class Batch:
    def __init__(self, copies, counted, sems, device):
        self.copies = copies
        self.whole = remote(counted, counted, sems, device)

    def start(self):
        for copy in self.copies:
            copy.start()

    def arrived(self):
        self.whole.wait_recv()

    def sent(self):
        self.whole.wait_send()


def halo_batch(sizes, buf, sems, same_slab):
    copies = []
    for direction in DIRECTIONS:
        dx, dy, dz = direction
        if (dx == 0) != same_slab:
            continue
        copies.append(
            remote(
                buf.at[pl.ds(1, 1), sent_part(dy), sent_part(dz)],
                buf.at[pl.ds(1 - dx, 1), landing_part(dy), landing_part(dz)],
                sems,
                neighbour(sizes, direction),
            )
        )
    counted = buf.at[1, pl.ds(0, 3)] if same_slab else buf.at[pl.ds(0, 2)]
    return Batch(copies, counted, sems, neighbour(sizes, (0, 0, 1)))


def tile_batch(sizes, buf, sems, tile, counted):
    ry, rz = RECEIVERS[tile]
    mine = buf.at[1, 1 + ry, 1 + rz]
    copies = []
    for dx in (-1, 0, 1):
        for dy, at_y in ((0, 1 + ry), (2 * ry - 1, 3 - 3 * ry)):
            for dz, at_z in ((0, 1 + rz), (2 * rz - 1, 3 - 3 * rz)):
                if (dx, dy, dz) != (0, 0, 0):
                    copies.append(
                        remote(
                            mine,
                            buf.at[1 - dx, at_y, at_z],
                            sems,
                            neighbour(sizes, (dx, dy, dz)),
                        )
                    )
    return Batch(copies, counted, sems, neighbour(sizes, (0, 0, 1)))


def group_steps(sizes, axes):
    steps = [()]
    for axis in axes:
        steps = [step + (n,) for step in steps for n in range(sizes[axis])]
    far = lambda step: sum(min(n, sizes[axis] - n) for n, axis in zip(step, axes))
    return sorted([step for step in steps if any(step)], key=far, reverse=True)


def group_batch(sizes, axes, buf, sems):
    me = 0
    for axis in axes:
        me = me * sizes[axis] + lax.axis_index(axis)
    copies = []
    for step in group_steps(sizes, axes):
        device = {axis: away(sizes, axis, n) for axis, n in zip(axes, step) if n != 0}
        copies.append(remote(buf.at[me], buf.at[me], sems, device))
    counted = buf.at[pl.ds(0, len(copies))]
    return me, Batch(copies, counted, sems, {axes[0]: away(sizes, axes[0], 1)})


def kernel(
    sizes,
    frac_hbm,
    pol_hbm,
    occ_hbm,
    mask_hbm,
    perm_hbm,
    hist_hbm,
    out_ref,
    change_ref,
    frac_ref,
    pol_ref,
    occ_ref,
    mask_ref,
    perm_ref,
    hist_ref,
    own_geo,
    geo,
    past,
    masked,
    moved_one,
    moved_two,
    perm_tiles,
    scaled_tiles,
    receiver,
    own_ends,
    ends,
    own_columns,
    columns,
    pairs,
    feats,
    partial,
    counted,
    in_sems,
    send_sems,
    recv_sems,
    *lines,
):
    lines_one, lines_two = lines[: len(FIRST_GROUPS)], lines[len(FIRST_GROUPS) :]
    sems = [(send_sems.at[n], recv_sems.at[n]) for n in range(SEMS)]

    loads = [
        pltpu.make_async_copy(src, dst, in_sems.at[n])
        for n, (src, dst) in enumerate(
            (
                (frac_hbm, frac_ref),
                (pol_hbm, pol_ref),
                (occ_hbm, occ_ref),
                (hist_hbm, hist_ref),
                (mask_hbm, mask_ref),
                (perm_hbm, perm_ref),
            )
        )
    ]
    for load in loads:
        load.start()

    barrier = pltpu.get_barrier_semaphore()
    greeted = []
    for axis in ("gz", "gx", "gy"):
        greeted += [
            {axis: away(sizes, axis, step)}
            for (step,) in group_steps(sizes, (axis,))
            if 2 <= step <= sizes[axis] - 2
        ]
    greeted += [neighbour(sizes, direction) for direction in DIRECTIONS]
    for device in greeted:
        pl.semaphore_signal(barrier, inc=1, device_id=device, device_id_type=MESH)

    lane = lax.broadcasted_iota(jnp.int32, (1, LANES), 1)
    sub = lax.broadcasted_iota(jnp.int32, (8, LANES), 0)
    lane16 = lax.broadcasted_iota(jnp.int32, (16, LANES), 1)
    sub16 = lax.broadcasted_iota(jnp.int32, (16, LANES), 0)

    loads[0].wait()
    loads[1].wait()
    for tile, (ry, rz) in enumerate(RECEIVERS):
        for which in range(2):
            for c in range(3):
                own_geo[tile, pl.ds(4 * which + c, 1)] = frac_ref[c, pl.ds(tile, 1), :]
            own_geo[tile, pl.ds(4 * which + 3, 1)] = pol_ref[pl.ds(tile, 1), :]
        geo[1, 1 + ry, 1 + rz] = own_geo[tile]

    def positions(slab, rows, sx, tile_y, tile_z):
        kind = lax.rem(rows, 4)
        shift = jnp.where(
            kind == 0,
            jnp.float32(sx - 1.5),
            jnp.where(kind == 1, (tile_y - 2).astype(F32), (tile_z - 2).astype(F32)),
        )
        at = (slab + shift) * CELL_EDGE
        return kind == 3, at, DAMP_ROOT * lax.rsqrt(slab)

    def squared(ref, first):
        parts = [ref[pl.ds(first + n, 1), :] for n in range(3)]
        return parts[0] * parts[0] + parts[1] * parts[1] + parts[2] * parts[2]

    row32 = lax.broadcasted_iota(jnp.int32, (32, LANES), 0)
    last, at, root = positions(
        own_geo[...].reshape(32, LANES), row32, 1, 1 + row32 // 16, 1 + lax.rem(row32 // 8, 2)
    )
    receiver[...] = jnp.where(last, -root, 2.0 * at)
    own_ends[...] = jnp.where(last, root, at)
    for tile in range(4):
        square = squared(own_ends, 8 * tile)
        receiver[pl.ds(8 * tile + 4, 1)] = square + SOFTENING
        own_ends[pl.ds(8 * tile + 4, 1)] = square
    own_columns[...] = jnp.transpose(
        jnp.concatenate([own_ends[...], jnp.zeros((96, LANES), F32)], axis=0)
    )

    def pair_factors(cols, places, offset_of, sx, first):
        for at, sy, sz in places:
            source = [
                jnp.broadcast_to(cols[:, at + n : at + n + 1], (16, LANES)) for n in range(5)
            ]
            for tile, (ry, rz) in enumerate(RECEIVERS):
                ky, kz = sy - ry, sz - rz
                if not (0 <= ky <= 2 and 0 <= kz <= 2):
                    continue
                damp = source[3] * receiver[pl.ds(8 * tile + 3, 1), :]
                dist = source[4] + receiver[pl.ds(8 * tile + 4, 1), :]
                for n in range(3):
                    dist = dist - source[n] * receiver[pl.ds(8 * tile + n, 1), :]
                offset = 9 * sx + 3 * ky + kz
                allowed = 3.0 * mask_ref[tile, offset].astype(F32)
                root = lax.rsqrt(dist)
                inverse = root * root
                cube = root * inverse * allowed
                if offset_of == "own" and ky == 1 and kz == 1:
                    cube = jnp.where(sub16 + first != lane16, cube, 0.0)
                power = dist * dist * root * damp
                fade = jnp.exp2(power)
                three = 1.0 - fade
                five = three + (power * LN2) * fade
                for part, value in ((0, five * (inverse * cube)), (128, three * cube)):
                    high = value.astype(BF16)
                    low = (value - high.astype(F32)).astype(BF16)
                    rows = pl.ds(pl.multiple_of(first + part, 16), 16)
                    pairs[tile, offset, rows, pl.ds(0, 128)] = high
                    pairs[tile, offset, rows, pl.ds(128, 128)] = low

    loads[2].wait()
    loads[3].wait()
    filled = occ_ref[...].astype(F32)
    filled_rows = jnp.concatenate([filled] * 6, axis=0)
    for h in range(6):
        masked[h] = hist_ref[h] * filled_rows
    row = jnp.zeros((1, LANES), F32)
    for a in range(6):
        for b in range(a, 6):
            product = masked[a] * masked[b]
            folded = product[0:8] + product[8:16] + product[16:24]
            value = jnp.sum(jnp.sum(folded, axis=0, keepdims=True), axis=1, keepdims=True)
            row = jnp.where(lane == 6 * a + b, value, row)

    own_places = [(8 * tile, 1 + ry, 1 + rz) for tile, (ry, rz) in enumerate(RECEIVERS)]
    all_places = [(8 * (4 * sy + sz), sy, sz) for sy in range(4) for sz in range(4)]
    rim_places = [(at, sy, sz) for at, sy, sz in all_places if sy in (0, 3) or sz in (0, 3)]

    def own_block(block, carry):
        for part in range(4):
            first = pl.multiple_of(block * 64 + part * 16, 16)
            pair_factors(own_columns[pl.ds(first, 16), :], own_places, "own", 1, first)
        return carry

    def clear(number, carry):
        sx, s = number // 16, lax.rem(number, 16)
        for piece in range(3):
            feats[sx, s, pl.ds(32 * piece, 16), pl.ds(128, 128)] = jnp.zeros((16, LANES), BF16)
        return carry

    def send_group(groups, number, bufs, first_sem, values):
        me, batch = group_batch(sizes, groups[number], bufs[number], sems[first_sem + number])
        bufs[number][me] = values
        batch.start()
        return batch

    def total(bufs, number, batch):
        batch.arrived()
        return jnp.sum(bufs[number][...], axis=0)

    pl.semaphore_wait(barrier, len(greeted))

    geo_batches = [halo_batch(sizes, geo, sems[n], n == 0) for n in range(2)]
    past_batches = [
        halo_batch(sizes, past, sems[2], True),
        Batch(
            [
                remote(past.at[1], past.at[1 - dx], sems[3], neighbour(sizes, (dx, 0, 0)))
                for dx in (-1, 1)
            ],
            past.at[pl.ds(0, 2)],
            sems[3],
            neighbour(sizes, (1, 0, 0)),
        ),
    ]
    line_a = send_group(FIRST_GROUPS, 0, lines_one, 8, row)
    for batch in geo_batches:
        batch.start()

    loads[4].wait()
    lax.fori_loop(0, 2, own_block, 0)
    for tile, (ry, rz) in enumerate(RECEIVERS):
        own = (1, 1 + ry, 1 + rz)
        for h in range(5):
            past[own + (pl.ds(6 * h, 6),)] = masked[h + 1, pl.ds(tile, 6, stride=4), :]
        past[own + (pl.ds(30, 2),)] = jnp.zeros((2, LANES), F32)

    row = total(lines_one, 0, line_a)
    line_b = send_group(FIRST_GROUPS, 1, lines_one, 8, row)
    past_batches[0].start()

    lax.fori_loop(0, 48, clear, 0, unroll=4)
    loads[5].wait()
    for tile in range(4):
        weight = jnp.broadcast_to(
            RELAXATION * occ_ref[pl.ds(tile, 1), :].astype(F32) * pol_ref[pl.ds(tile, 1), :],
            (8, LANES),
        )
        scaled_tiles[tile] = jnp.where(lax.rem(sub, 4) == 3, 0.0, weight)
        perm_tiles[tile] = jnp.zeros((8, LANES), F32)
        for which in range(2):
            perm_tiles[tile, pl.ds(4 * which, 3), :] = perm_ref[
                pl.ds(12 * which + tile, 3, stride=4), :
            ]

    row128 = lax.broadcasted_iota(jnp.int32, (LANES, LANES), 0)

    def place_slab(sx):
        last, at, root = positions(
            geo[sx].reshape(LANES, LANES), row128, sx, row128 // 32, lax.rem(row128 // 8, 4)
        )
        ends[sx] = jnp.where(last, 1.0, at)
        lengths = at * at
        lengths = (
            lengths
            + pltpu.roll(lengths, LANES - 1, 0)
            + pltpu.roll(lengths, LANES - 2, 0)
        )
        columns[sx] = jnp.transpose(
            jnp.where(lax.rem(row128, 8) == 4, lengths, jnp.where(last, root, at))
        )

    geo_batches[0].arrived()
    place_slab(1)

    def rim_block(block, carry):
        for part in range(4):
            first = pl.multiple_of(block * 64 + part * 16, 16)
            pair_factors(columns[1, pl.ds(first, 16), :], rim_places, "rim", 1, first)
        return carry

    lax.fori_loop(0, 2, rim_block, 0)

    past_batches[0].arrived()
    past_batches[1].start()
    geo_batches[1].arrived()
    place_slab(0)
    place_slab(2)

    def side_block(step, carry):
        sx = 2 * (step // 4)
        for part in range(2):
            first = pl.multiple_of(lax.rem(step, 4) * 32 + part * 16, 16)
            pair_factors(columns[sx, pl.ds(first, 16), :], all_places, "side", sx, first)
        return carry

    lax.fori_loop(0, 3, side_block, 0)
    row = total(lines_one, 1, line_b)
    line_c = send_group(FIRST_GROUPS, 2, lines_one, 8, row)
    lax.fori_loop(3, 8, side_block, 0)
    row = total(lines_one, 2, line_c)

    def entry(a, b):
        return jnp.sum(
            jnp.where(lane == 6 * min(a, b) + max(a, b), row, 0.0), axis=1, keepdims=True
        )

    gram = {(a, b): entry(a, b) for a in range(6) for b in range(a, 6) if a < 5}
    trace = gram[0, 0] + gram[1, 1] + gram[2, 2] + gram[3, 3] + gram[4, 4]
    ridge = 0.001 * trace / 5.0 + 1.0
    low = {}
    scale = []
    half = []
    for a in range(5):
        pivot = gram[a, a] + ridge
        for c in range(a):
            pivot = pivot - low[a, c] * low[a, c]
        scale.append(lax.rsqrt(pivot))
        for b in range(a + 1, 5):
            value = gram[a, b]
            for c in range(a):
                value = value - low[a, c] * low[b, c]
            low[b, a] = value * scale[a]
        value = gram[a, 5]
        for c in range(a):
            value = value - low[a, c] * half[c]
        half.append(value * scale[a])
    coeffs = [None] * 5
    for a in reversed(range(5)):
        value = half[a]
        for b in range(a + 1, 5):
            value = value - low[b, a] * coeffs[b]
        coeffs[a] = value * scale[a]
    coeffs = [jnp.broadcast_to(value, (8, LANES))[0:6] for value in coeffs]

    past_batches[1].arrived()

    first_set = sub < 4
    flat = jnp.zeros((8, LANES), F32)

    def write_feats(sx, s, tile_ref):
        whole = tile_ref[...]
        near = ends[sx, pl.ds(8 * s, 8), :]
        multipliers = []
        along = None
        for b in range(3):
            both = jnp.where(first_set, whole[b : b + 1], whole[4 + b : 5 + b])
            multipliers.append(both)
            term = near[b : b + 1] * both
            along = term if along is None else along + term
        multipliers.append(along)
        parts = [near * value for value in multipliers]
        for half_at in range(2):
            value = jnp.concatenate(parts[2 * half_at : 2 * half_at + 2], axis=0)
            for piece in range(3):
                kept = value.astype(BF16)
                feats[sx, s, pl.ds(32 * piece + 16 * half_at, 16), pl.ds(0, 128)] = kept
                value = value - kept.astype(F32)
        value = jnp.concatenate([flat, whole * (-1.0 / 3.0)], axis=0)
        for piece in range(3):
            kept = value.astype(BF16)
            feats[sx, s, pl.ds(32 * piece + 16, 16), pl.ds(128, 128)] = kept
            value = value - kept.astype(F32)

    def predict(sx, carry):
        for s in range(16):
            sy, sz = s // 4, s % 4
            value = None
            for h in range(5):
                term = coeffs[h] * past[sx, sy, sz, pl.ds(6 * h, 6), :]
                value = term if value is None else value + term
            moved_one[sx, sy, sz] = flat
            moved_one[sx, sy, sz, pl.ds(0, 3), :] = value[0:3]
            moved_one[sx, sy, sz, pl.ds(4, 3), :] = value[3:6]
        for s in range(16):
            write_feats(sx, s, moved_one.at[sx, s // 4, s % 4])
        return carry

    lax.fori_loop(0, 3, predict, 0)

    def dot_part(tile, sources):
        if len(sources) > 6:
            middle = len(sources) // 2
            return dot_piece(tile, sources[:middle]) + dot_piece(tile, sources[middle:])
        return dot_piece(tile, sources)

    def joined(summed):
        both = summed[:, 0:128] + summed[:, 128:256]
        return both[0:32] + both[32:64] + both[64:96]

    def dot_piece(tile, sources):
        ry, rz = RECEIVERS[tile]
        lhs = jnp.concatenate([feats[sx, 4 * sy + sz] for sx, sy, sz in sources], axis=1)
        rhs = jnp.concatenate(
            [pairs[tile, 9 * sx + 3 * (sy - ry) + sz - rz] for sx, sy, sz in sources], axis=0
        )
        return joined(jnp.dot(lhs, rhs, preferred_element_type=F32))

    def sources_of(tile, kinds=None):
        ry, rz = RECEIVERS[tile]
        return [
            (sx, ry + ky, rz + kz)
            for sx in range(3)
            for ky in range(3)
            for kz in range(3)
            if kinds is None or ((ry + ky + 1) % 2, (rz + kz + 1) % 2) == kinds
        ]

    def relaxed(tile, before, out):
        ry, rz = RECEIVERS[tile]
        here = ends[1, pl.ds(8 * (4 * (ry + 1) + rz + 1), 8), :]
        value = out[24:32]
        for b in range(3):
            value = value - here[b : b + 1] * out[8 * b : 8 * b + 8]
        shared = jnp.where(first_set, value[3:4], value[7:8])
        field = value - here * shared
        return (1.0 - RELAXATION) * before + scaled_tiles[tile] * (perm_tiles[tile] + field)

    tile_batches = []
    summed = dot_part(0, sources_of(0))
    for tile, (ry, rz) in enumerate(RECEIVERS):
        now = summed
        if tile < 3:
            summed = dot_part(tile + 1, sources_of(tile + 1))
        before = moved_one[1, 1 + ry, 1 + rz]
        moved_two[1, 1 + ry, 1 + rz] = relaxed(tile, before, now)
        tile_batches.append(tile_batch(sizes, moved_two, sems[4 + tile], tile, counted))
        tile_batches[-1].start()

    for batch in geo_batches + past_batches + [line_a, line_b, line_c]:
        batch.sent()

    changed = flat
    size = flat
    for kind, kinds in enumerate(RECEIVERS):
        tile_batches[kind].arrived()
        tiles = [
            (sy, sz)
            for sy in range(4)
            for sz in range(4)
            if ((sy + 1) % 2, (sz + 1) % 2) == kinds
        ]
        for sx in range(3):
            for sy, sz in tiles:
                write_feats(sx, 4 * sy + sz, moved_two.at[sx, sy, sz])
        for tile, (ry, rz) in enumerate(RECEIVERS):
            summed = dot_part(tile, sources_of(tile, kinds))
            if kind > 0:
                summed = summed + partial[tile]
            if kind < 3:
                partial[tile] = summed
                continue
            before = moved_two[1, 1 + ry, 1 + rz]
            after = relaxed(tile, before, summed)
            out_ref[pl.ds(tile, 3, stride=4), :] = after[0:3]
            out_ref[pl.ds(12 + tile, 3, stride=4), :] = after[4:7]
            update = after - before
            changed = changed + update * update
            size = size + after * after

    def whole_sum(value):
        return jnp.sum(jnp.sum(value, axis=0, keepdims=True), axis=1, keepdims=True)

    row = jnp.where(lane == 0, whole_sum(changed), jnp.where(lane == 1, whole_sum(size), 0.0))
    ending = []
    for number in range(len(LAST_GROUPS)):
        ending.append(send_group(LAST_GROUPS, number, lines_two, 8 + len(FIRST_GROUPS), row))
        if number == 0:
            for batch in tile_batches:
                batch.sent()
        row = total(lines_two, number, ending[-1])
    top = jnp.sum(jnp.where(lane == 0, row, 0.0), axis=1, keepdims=True)
    bottom = jnp.sum(jnp.where(lane == 1, row, 0.0), axis=1, keepdims=True)
    change_ref[...] = jnp.broadcast_to(jnp.sqrt(top / (bottom + 1.0)), (1, LANES))

    for batch in ending:
        batch.sent()


def in_hbm(array):
    return pltpu.with_memory_space_constraint(array, pltpu.HBM)


def on_device(sizes, fractions, polarizability, occupancy, pair_mask, perm_field, history):
    vmem = pl.BlockSpec(memory_space=pltpu.VMEM)
    hbm = pl.BlockSpec(memory_space=pltpu.HBM)
    dma = pltpu.SemaphoreType.DMA
    line_bufs = [
        pltpu.VMEM((math.prod(sizes[axis] for axis in axes), 1, LANES), F32)
        for axes in FIRST_GROUPS + LAST_GROUPS
    ]
    scratch = [
        pltpu.VMEM((3, 4, LANES), F32),
        pltpu.VMEM((4, LANES), F32),
        pltpu.VMEM((4, LANES), jnp.int32),
        pltpu.SMEM((4, 27), jnp.int32),
        pltpu.VMEM((24, LANES), F32),
        pltpu.VMEM((6, 24, LANES), F32),
        pltpu.VMEM((4, 8, LANES), F32),
        pltpu.VMEM((3, 4, 4, 8, LANES), F32),
        pltpu.VMEM((3, 4, 4, 32, LANES), F32),
        pltpu.VMEM((6, 24, LANES), F32),
        pltpu.VMEM((3, 4, 4, 8, LANES), F32),
        pltpu.VMEM((3, 4, 4, 8, LANES), F32),
        pltpu.VMEM((4, 8, LANES), F32),
        pltpu.VMEM((4, 8, LANES), F32),
        pltpu.VMEM((32, LANES), F32),
        pltpu.VMEM((32, LANES), F32),
        pltpu.VMEM((3, LANES, LANES), F32),
        pltpu.VMEM((LANES, LANES), F32),
        pltpu.VMEM((3, LANES, LANES), F32),
        pltpu.VMEM((4, 27, 256, 256), BF16),
        pltpu.VMEM((3, 16, 96, 256), BF16),
        pltpu.VMEM((4, 32, LANES), F32),
        pltpu.VMEM((11, 8, LANES), F32),
        dma((6,)),
        dma((SEMS,)),
        dma((SEMS,)),
    ]
    induced, change = pl.pallas_call(
        lambda *refs: kernel(sizes, *refs),
        out_shape=(
            jax.ShapeDtypeStruct((24, LANES), F32),
            jax.ShapeDtypeStruct((1, LANES), F32),
        ),
        in_specs=[hbm] * 6,
        out_specs=(vmem, vmem),
        scratch_shapes=scratch + line_bufs,
        compiler_params=pltpu.CompilerParams(
            collective_id=0, has_side_effects=True, vmem_limit_bytes=VMEM_BYTES
        ),
    )(
        in_hbm(fractions.reshape(3, 4, LANES)),
        in_hbm(polarizability.reshape(4, LANES)),
        in_hbm(occupancy.reshape(4, LANES)),
        in_hbm(pair_mask.reshape(4, 27)),
        in_hbm(perm_field.reshape(24, LANES)),
        in_hbm(history.reshape(6, 24, LANES)),
    )
    return induced.reshape(6, 1, 2, 2, LANES), change[0, 0]


def solution(mesh):
    sizes = {axis: mesh.shape[axis] for axis in AXES}
    placed = (
        P(None, "gx", "gy", "gz", None),
        P("gx", "gy", "gz", None),
        P("gx", "gy", "gz", None),
        P("gx", "gy", "gz", None),
        P(None, "gx", "gy", "gz", None),
        P(None, None, "gx", "gy", "gz", None),
    )
    return jax.shard_map(
        lambda *args: on_device(sizes, *args),
        mesh=mesh,
        in_specs=placed,
        out_specs=(P(None, "gx", "gy", "gz", None), P()),
        check_vma=False,
    )
```

```python
import math

import jax
import jax.numpy as jnp
from jax import lax
from jax.experimental import pallas as pl
from jax.experimental.pallas import tpu as pltpu
from jax.sharding import PartitionSpec as P

AXES = ("gx", "gy", "gz")
FIRST_GROUPS = (("gy",), ("gx",), ("gz",))
LAST_GROUPS = (("gx",), ("gy", "gz"))
MESH = pl.DeviceIdType.MESH
F32 = jnp.float32
BF16 = jnp.bfloat16
LANES = 128
DIRECTIONS = [
    (dx, dy, dz)
    for dx in (-1, 0, 1)
    for dy in (-1, 0, 1)
    for dz in (-1, 0, 1)
    if (dx, dy, dz) != (0, 0, 0)
]
CELL_EDGE = 10.0
SOFTENING = 0.3
THOLE_DAMP = 0.39
RELAXATION = 0.7
LN2 = math.log(2.0)
DAMP_ROOT = math.sqrt(THOLE_DAMP / LN2)
RECEIVERS = [(ry, rz) for ry in (0, 1) for rz in (0, 1)]


SEMS = 8 + len(FIRST_GROUPS) + len(LAST_GROUPS)
VMEM_BYTES = 40 * 1024 * 1024


def away(sizes, axis, step):
    return lax.rem(lax.axis_index(axis) + (step + sizes[axis]), sizes[axis])


def neighbour(sizes, direction):
    return {axis: away(sizes, axis, step) for axis, step in zip(AXES, direction) if step != 0}


def sent_part(step):
    return {0: pl.ds(1, 2), 1: pl.ds(2, 1), -1: pl.ds(1, 1)}[step]


def landing_part(step):
    return {0: pl.ds(1, 2), 1: pl.ds(0, 1), -1: pl.ds(3, 1)}[step]


def remote(src, dst, sems, device):
    return pltpu.make_async_remote_copy(
        src_ref=src,
        dst_ref=dst,
        send_sem=sems[0],
        recv_sem=sems[1],
        device_id=device,
        device_id_type=MESH,
    )


class Batch:
    def __init__(self, copies, counted, sems, device):
        self.copies = copies
        self.whole = remote(counted, counted, sems, device)

    def start(self):
        for copy in self.copies:
            copy.start()

    def arrived(self):
        self.whole.wait_recv()

    def sent(self):
        self.whole.wait_send()


def halo_batch(sizes, buf, sems, same_slab):
    copies = []
    for direction in DIRECTIONS:
        dx, dy, dz = direction
        if (dx == 0) != same_slab:
            continue
        copies.append(
            remote(
                buf.at[pl.ds(1, 1), sent_part(dy), sent_part(dz)],
                buf.at[pl.ds(1 - dx, 1), landing_part(dy), landing_part(dz)],
                sems,
                neighbour(sizes, direction),
            )
        )
    counted = buf.at[1, pl.ds(0, 3)] if same_slab else buf.at[pl.ds(0, 2)]
    return Batch(copies, counted, sems, neighbour(sizes, (0, 0, 1)))


def tile_batch(sizes, buf, sems, tile, counted):
    ry, rz = RECEIVERS[tile]
    mine = buf.at[1, 1 + ry, 1 + rz]
    copies = []
    for dx in (-1, 0, 1):
        for dy, at_y in ((0, 1 + ry), (2 * ry - 1, 3 - 3 * ry)):
            for dz, at_z in ((0, 1 + rz), (2 * rz - 1, 3 - 3 * rz)):
                if (dx, dy, dz) != (0, 0, 0):
                    copies.append(
                        remote(
                            mine,
                            buf.at[1 - dx, at_y, at_z],
                            sems,
                            neighbour(sizes, (dx, dy, dz)),
                        )
                    )
    return Batch(copies, counted, sems, neighbour(sizes, (0, 0, 1)))


def group_steps(sizes, axes):
    steps = [()]
    for axis in axes:
        steps = [step + (n,) for step in steps for n in range(sizes[axis])]
    far = lambda step: sum(min(n, sizes[axis] - n) for n, axis in zip(step, axes))
    return sorted([step for step in steps if any(step)], key=far, reverse=True)


def group_batch(sizes, axes, buf, sems):
    me = 0
    for axis in axes:
        me = me * sizes[axis] + lax.axis_index(axis)
    copies = []
    for step in group_steps(sizes, axes):
        device = {axis: away(sizes, axis, n) for axis, n in zip(axes, step) if n != 0}
        copies.append(remote(buf.at[me], buf.at[me], sems, device))
    counted = buf.at[pl.ds(0, len(copies))]
    return me, Batch(copies, counted, sems, {axes[0]: away(sizes, axes[0], 1)})


def kernel(
    sizes,
    frac_hbm,
    pol_hbm,
    occ_hbm,
    mask_hbm,
    perm_hbm,
    hist_hbm,
    out_ref,
    change_ref,
    frac_ref,
    pol_ref,
    occ_ref,
    mask_ref,
    perm_ref,
    hist_ref,
    own_geo,
    geo,
    past,
    masked,
    moved_one,
    moved_two,
    perm_tiles,
    scaled_tiles,
    receiver,
    own_ends,
    ends,
    own_columns,
    columns,
    pairs,
    feats,
    partial,
    counted,
    in_sems,
    send_sems,
    recv_sems,
    *lines,
):
    lines_one, lines_two = lines[: len(FIRST_GROUPS)], lines[len(FIRST_GROUPS) :]
    sems = [(send_sems.at[n], recv_sems.at[n]) for n in range(SEMS)]

    loads = [
        pltpu.make_async_copy(src, dst, in_sems.at[n])
        for n, (src, dst) in enumerate(
            (
                (frac_hbm, frac_ref),
                (pol_hbm, pol_ref),
                (occ_hbm, occ_ref),
                (hist_hbm, hist_ref),
                (mask_hbm, mask_ref),
                (perm_hbm, perm_ref),
            )
        )
    ]
    for load in loads:
        load.start()

    barrier = pltpu.get_barrier_semaphore()
    greeted = []
    for axis in ("gz", "gx", "gy"):
        greeted += [
            {axis: away(sizes, axis, step)}
            for (step,) in group_steps(sizes, (axis,))
            if 2 <= step <= sizes[axis] - 2
        ]
    greeted += [neighbour(sizes, direction) for direction in DIRECTIONS]
    for device in greeted:
        pl.semaphore_signal(barrier, inc=1, device_id=device, device_id_type=MESH)

    lane = lax.broadcasted_iota(jnp.int32, (1, LANES), 1)
    sub = lax.broadcasted_iota(jnp.int32, (8, LANES), 0)
    lane16 = lax.broadcasted_iota(jnp.int32, (16, LANES), 1)
    sub16 = lax.broadcasted_iota(jnp.int32, (16, LANES), 0)

    loads[0].wait()
    loads[1].wait()
    for tile, (ry, rz) in enumerate(RECEIVERS):
        for which in range(2):
            for c in range(3):
                own_geo[tile, pl.ds(4 * which + c, 1)] = frac_ref[c, pl.ds(tile, 1), :]
            own_geo[tile, pl.ds(4 * which + 3, 1)] = pol_ref[pl.ds(tile, 1), :]
        geo[1, 1 + ry, 1 + rz] = own_geo[tile]

    def positions(slab, rows, sx, tile_y, tile_z):
        kind = lax.rem(rows, 4)
        shift = jnp.where(
            kind == 0,
            jnp.float32(sx - 1.5),
            jnp.where(kind == 1, (tile_y - 2).astype(F32), (tile_z - 2).astype(F32)),
        )
        at = (slab + shift) * CELL_EDGE
        return kind == 3, at, DAMP_ROOT * lax.rsqrt(slab)

    def squared(ref, first):
        parts = [ref[pl.ds(first + n, 1), :] for n in range(3)]
        return parts[0] * parts[0] + parts[1] * parts[1] + parts[2] * parts[2]

    row32 = lax.broadcasted_iota(jnp.int32, (32, LANES), 0)
    last, at, root = positions(
        own_geo[...].reshape(32, LANES), row32, 1, 1 + row32 // 16, 1 + lax.rem(row32 // 8, 2)
    )
    receiver[...] = jnp.where(last, -root, 2.0 * at)
    own_ends[...] = jnp.where(last, root, at)
    for tile in range(4):
        square = squared(own_ends, 8 * tile)
        receiver[pl.ds(8 * tile + 4, 1)] = square + SOFTENING
        own_ends[pl.ds(8 * tile + 4, 1)] = square
    own_columns[...] = jnp.transpose(
        jnp.concatenate([own_ends[...], jnp.zeros((96, LANES), F32)], axis=0)
    )

    def pair_factors(cols, places, offset_of, sx, first):
        for at, sy, sz in places:
            source = [
                jnp.broadcast_to(cols[:, at + n : at + n + 1], (16, LANES)) for n in range(5)
            ]
            for tile, (ry, rz) in enumerate(RECEIVERS):
                ky, kz = sy - ry, sz - rz
                if not (0 <= ky <= 2 and 0 <= kz <= 2):
                    continue
                damp = source[3] * receiver[pl.ds(8 * tile + 3, 1), :]
                dist = source[4] + receiver[pl.ds(8 * tile + 4, 1), :]
                for n in range(3):
                    dist = dist - source[n] * receiver[pl.ds(8 * tile + n, 1), :]
                offset = 9 * sx + 3 * ky + kz
                allowed = 3.0 * mask_ref[tile, offset].astype(F32)
                root = lax.rsqrt(dist)
                inverse = root * root
                cube = root * inverse * allowed
                if offset_of == "own" and ky == 1 and kz == 1:
                    cube = jnp.where(sub16 + first != lane16, cube, 0.0)
                power = dist * dist * root * damp
                fade = jnp.exp2(power)
                three = 1.0 - fade
                five = three + (power * LN2) * fade
                for part, value in ((0, five * (inverse * cube)), (128, three * cube)):
                    high = value.astype(BF16)
                    low = (value - high.astype(F32)).astype(BF16)
                    rows = pl.ds(pl.multiple_of(first + part, 16), 16)
                    pairs[tile, offset, rows, pl.ds(0, 128)] = high
                    pairs[tile, offset, rows, pl.ds(128, 128)] = low

    loads[2].wait()
    loads[3].wait()
    filled = occ_ref[...].astype(F32)
    filled_rows = jnp.concatenate([filled] * 6, axis=0)
    for h in range(6):
        masked[h] = hist_ref[h] * filled_rows
    row = jnp.zeros((1, LANES), F32)
    for a in range(6):
        for b in range(a, 6):
            product = masked[a] * masked[b]
            folded = product[0:8] + product[8:16] + product[16:24]
            value = jnp.sum(jnp.sum(folded, axis=0, keepdims=True), axis=1, keepdims=True)
            row = jnp.where(lane == 6 * a + b, value, row)

    for tile, (ry, rz) in enumerate(RECEIVERS):
        own = (1, 1 + ry, 1 + rz)
        for h in range(5):
            past[own + (pl.ds(6 * h, 6),)] = masked[h + 1, pl.ds(tile, 6, stride=4), :]
        past[own + (pl.ds(30, 2),)] = jnp.zeros((2, LANES), F32)

    own_places = [(8 * tile, 1 + ry, 1 + rz) for tile, (ry, rz) in enumerate(RECEIVERS)]
    all_places = [(8 * (4 * sy + sz), sy, sz) for sy in range(4) for sz in range(4)]
    rim_places = [(at, sy, sz) for at, sy, sz in all_places if sy in (0, 3) or sz in (0, 3)]

    def own_block(block, carry):
        for part in range(4):
            first = pl.multiple_of(block * 64 + part * 16, 16)
            pair_factors(own_columns[pl.ds(first, 16), :], own_places, "own", 1, first)
        return carry

    def clear(number, carry):
        sx, s = number // 16, lax.rem(number, 16)
        for piece in range(3):
            feats[sx, s, pl.ds(32 * piece, 16), pl.ds(128, 128)] = jnp.zeros((16, LANES), BF16)
        return carry

    def send_group(groups, number, bufs, first_sem, values):
        me, batch = group_batch(sizes, groups[number], bufs[number], sems[first_sem + number])
        bufs[number][me] = values
        batch.start()
        return batch

    def total(bufs, number, batch):
        batch.arrived()
        return jnp.sum(bufs[number][...], axis=0)

    pl.semaphore_wait(barrier, len(greeted))

    geo_batches = [halo_batch(sizes, geo, sems[n], n == 0) for n in range(2)]
    past_batches = [
        halo_batch(sizes, past, sems[2], True),
        Batch(
            [
                remote(past.at[1], past.at[1 - dx], sems[3], neighbour(sizes, (dx, 0, 0)))
                for dx in (-1, 1)
            ],
            past.at[pl.ds(0, 2)],
            sems[3],
            neighbour(sizes, (1, 0, 0)),
        ),
    ]
    line_a = send_group(FIRST_GROUPS, 0, lines_one, 8, row)
    for batch in geo_batches:
        batch.start()
    past_batches[0].start()

    loads[4].wait()
    lax.fori_loop(0, 2, own_block, 0)

    row = total(lines_one, 0, line_a)
    line_b = send_group(FIRST_GROUPS, 1, lines_one, 8, row)

    lax.fori_loop(0, 48, clear, 0, unroll=4)
    loads[5].wait()
    for tile in range(4):
        weight = jnp.broadcast_to(
            RELAXATION * occ_ref[pl.ds(tile, 1), :].astype(F32) * pol_ref[pl.ds(tile, 1), :],
            (8, LANES),
        )
        scaled_tiles[tile] = jnp.where(lax.rem(sub, 4) == 3, 0.0, weight)
        perm_tiles[tile] = jnp.zeros((8, LANES), F32)
        for which in range(2):
            perm_tiles[tile, pl.ds(4 * which, 3), :] = perm_ref[
                pl.ds(12 * which + tile, 3, stride=4), :
            ]

    row128 = lax.broadcasted_iota(jnp.int32, (LANES, LANES), 0)

    def place_slab(sx):
        last, at, root = positions(
            geo[sx].reshape(LANES, LANES), row128, sx, row128 // 32, lax.rem(row128 // 8, 4)
        )
        ends[sx] = jnp.where(last, 1.0, at)
        lengths = at * at
        lengths = (
            lengths
            + pltpu.roll(lengths, LANES - 1, 0)
            + pltpu.roll(lengths, LANES - 2, 0)
        )
        columns[sx] = jnp.transpose(
            jnp.where(lax.rem(row128, 8) == 4, lengths, jnp.where(last, root, at))
        )

    geo_batches[0].arrived()
    place_slab(1)

    def rim_block(block, carry):
        for part in range(4):
            first = pl.multiple_of(block * 64 + part * 16, 16)
            pair_factors(columns[1, pl.ds(first, 16), :], rim_places, "rim", 1, first)
        return carry

    lax.fori_loop(0, 2, rim_block, 0)

    past_batches[0].arrived()
    past_batches[1].start()
    geo_batches[1].arrived()
    place_slab(0)
    place_slab(2)

    def side_block(step, carry):
        sx = 2 * (step // 2)
        for part in range(4):
            first = pl.multiple_of(lax.rem(step, 2) * 64 + part * 16, 16)
            pair_factors(columns[sx, pl.ds(first, 16), :], all_places, "side", sx, first)
        return carry

    lax.fori_loop(0, 1, side_block, 0)
    row = total(lines_one, 1, line_b)
    line_c = send_group(FIRST_GROUPS, 2, lines_one, 8, row)
    lax.fori_loop(1, 4, side_block, 0)
    row = total(lines_one, 2, line_c)

    def entry(a, b):
        return jnp.sum(
            jnp.where(lane == 6 * min(a, b) + max(a, b), row, 0.0), axis=1, keepdims=True
        )

    gram = {(a, b): entry(a, b) for a in range(6) for b in range(a, 6) if a < 5}
    trace = gram[0, 0] + gram[1, 1] + gram[2, 2] + gram[3, 3] + gram[4, 4]
    ridge = 0.001 * trace / 5.0 + 1.0
    low = {}
    scale = []
    half = []
    for a in range(5):
        pivot = gram[a, a] + ridge
        for c in range(a):
            pivot = pivot - low[a, c] * low[a, c]
        scale.append(lax.rsqrt(pivot))
        for b in range(a + 1, 5):
            value = gram[a, b]
            for c in range(a):
                value = value - low[a, c] * low[b, c]
            low[b, a] = value * scale[a]
        value = gram[a, 5]
        for c in range(a):
            value = value - low[a, c] * half[c]
        half.append(value * scale[a])
    coeffs = [None] * 5
    for a in reversed(range(5)):
        value = half[a]
        for b in range(a + 1, 5):
            value = value - low[b, a] * coeffs[b]
        coeffs[a] = value * scale[a]
    coeffs = [jnp.broadcast_to(value, (8, LANES))[0:6] for value in coeffs]

    past_batches[1].arrived()

    first_set = sub < 4
    flat = jnp.zeros((8, LANES), F32)

    def write_feats(sx, s, tile_ref):
        whole = tile_ref[...]
        near = ends[sx, pl.ds(8 * s, 8), :]
        multipliers = []
        along = None
        for b in range(3):
            both = jnp.where(first_set, whole[b : b + 1], whole[4 + b : 5 + b])
            multipliers.append(both)
            term = near[b : b + 1] * both
            along = term if along is None else along + term
        multipliers.append(along)
        parts = [near * value for value in multipliers]
        for half_at in range(2):
            value = jnp.concatenate(parts[2 * half_at : 2 * half_at + 2], axis=0)
            for piece in range(3):
                kept = value.astype(BF16)
                feats[sx, s, pl.ds(32 * piece + 16 * half_at, 16), pl.ds(0, 128)] = kept
                value = value - kept.astype(F32)
        value = jnp.concatenate([flat, whole * (-1.0 / 3.0)], axis=0)
        for piece in range(3):
            kept = value.astype(BF16)
            feats[sx, s, pl.ds(32 * piece + 16, 16), pl.ds(128, 128)] = kept
            value = value - kept.astype(F32)

    def predict(sx, carry):
        for s in range(16):
            sy, sz = s // 4, s % 4
            value = None
            for h in range(5):
                term = coeffs[h] * past[sx, sy, sz, pl.ds(6 * h, 6), :]
                value = term if value is None else value + term
            moved_one[sx, sy, sz] = flat
            moved_one[sx, sy, sz, pl.ds(0, 3), :] = value[0:3]
            moved_one[sx, sy, sz, pl.ds(4, 3), :] = value[3:6]
        for s in range(16):
            write_feats(sx, s, moved_one.at[sx, s // 4, s % 4])
        return carry

    lax.fori_loop(0, 3, predict, 0)

    def dot_part(tile, sources):
        if len(sources) > 6:
            middle = len(sources) // 2
            return dot_piece(tile, sources[:middle]) + dot_piece(tile, sources[middle:])
        return dot_piece(tile, sources)

    def joined(summed):
        both = summed[:, 0:128] + summed[:, 128:256]
        return both[0:32] + both[32:64] + both[64:96]

    def dot_piece(tile, sources):
        ry, rz = RECEIVERS[tile]
        lhs = jnp.concatenate([feats[sx, 4 * sy + sz] for sx, sy, sz in sources], axis=1)
        rhs = jnp.concatenate(
            [pairs[tile, 9 * sx + 3 * (sy - ry) + sz - rz] for sx, sy, sz in sources], axis=0
        )
        return joined(jnp.dot(lhs, rhs, preferred_element_type=F32))

    def sources_of(tile, kinds=None):
        ry, rz = RECEIVERS[tile]
        return [
            (sx, ry + ky, rz + kz)
            for sx in range(3)
            for ky in range(3)
            for kz in range(3)
            if kinds is None or ((ry + ky + 1) % 2, (rz + kz + 1) % 2) == kinds
        ]

    def relaxed(tile, before, out):
        ry, rz = RECEIVERS[tile]
        here = ends[1, pl.ds(8 * (4 * (ry + 1) + rz + 1), 8), :]
        value = out[24:32]
        for b in range(3):
            value = value - here[b : b + 1] * out[8 * b : 8 * b + 8]
        shared = jnp.where(first_set, value[3:4], value[7:8])
        field = value - here * shared
        return (1.0 - RELAXATION) * before + scaled_tiles[tile] * (perm_tiles[tile] + field)

    tile_batches = []
    summed = dot_part(0, sources_of(0))
    for tile, (ry, rz) in enumerate(RECEIVERS):
        now = summed
        if tile < 3:
            summed = dot_part(tile + 1, sources_of(tile + 1))
        before = moved_one[1, 1 + ry, 1 + rz]
        moved_two[1, 1 + ry, 1 + rz] = relaxed(tile, before, now)
        tile_batches.append(tile_batch(sizes, moved_two, sems[4 + tile], tile, counted))
        tile_batches[-1].start()

    for batch in geo_batches + past_batches + [line_a, line_b, line_c]:
        batch.sent()

    changed = flat
    size = flat
    for kind, kinds in enumerate(RECEIVERS):
        tile_batches[kind].arrived()
        tiles = [
            (sy, sz)
            for sy in range(4)
            for sz in range(4)
            if ((sy + 1) % 2, (sz + 1) % 2) == kinds
        ]
        for sx in range(3):
            for sy, sz in tiles:
                write_feats(sx, 4 * sy + sz, moved_two.at[sx, sy, sz])
        for tile, (ry, rz) in enumerate(RECEIVERS):
            summed = dot_part(tile, sources_of(tile, kinds))
            if kind > 0:
                summed = summed + partial[tile]
            if kind < 3:
                partial[tile] = summed
                continue
            before = moved_two[1, 1 + ry, 1 + rz]
            after = relaxed(tile, before, summed)
            out_ref[pl.ds(tile, 3, stride=4), :] = after[0:3]
            out_ref[pl.ds(12 + tile, 3, stride=4), :] = after[4:7]
            update = after - before
            changed = changed + update * update
            size = size + after * after

    def whole_sum(value):
        return jnp.sum(jnp.sum(value, axis=0, keepdims=True), axis=1, keepdims=True)

    row = jnp.where(lane == 0, whole_sum(changed), jnp.where(lane == 1, whole_sum(size), 0.0))
    ending = []
    for number in range(len(LAST_GROUPS)):
        ending.append(send_group(LAST_GROUPS, number, lines_two, 8 + len(FIRST_GROUPS), row))
        if number == 0:
            for batch in tile_batches:
                batch.sent()
        row = total(lines_two, number, ending[-1])
    top = jnp.sum(jnp.where(lane == 0, row, 0.0), axis=1, keepdims=True)
    bottom = jnp.sum(jnp.where(lane == 1, row, 0.0), axis=1, keepdims=True)
    change_ref[...] = jnp.broadcast_to(jnp.sqrt(top / (bottom + 1.0)), (1, LANES))

    for batch in ending:
        batch.sent()


def in_hbm(array):
    return pltpu.with_memory_space_constraint(array, pltpu.HBM)


def on_device(sizes, fractions, polarizability, occupancy, pair_mask, perm_field, history):
    vmem = pl.BlockSpec(memory_space=pltpu.VMEM)
    hbm = pl.BlockSpec(memory_space=pltpu.HBM)
    dma = pltpu.SemaphoreType.DMA
    line_bufs = [
        pltpu.VMEM((math.prod(sizes[axis] for axis in axes), 1, LANES), F32)
        for axes in FIRST_GROUPS + LAST_GROUPS
    ]
    scratch = [
        pltpu.VMEM((3, 4, LANES), F32),
        pltpu.VMEM((4, LANES), F32),
        pltpu.VMEM((4, LANES), jnp.int32),
        pltpu.SMEM((4, 27), jnp.int32),
        pltpu.VMEM((24, LANES), F32),
        pltpu.VMEM((6, 24, LANES), F32),
        pltpu.VMEM((4, 8, LANES), F32),
        pltpu.VMEM((3, 4, 4, 8, LANES), F32),
        pltpu.VMEM((3, 4, 4, 32, LANES), F32),
        pltpu.VMEM((6, 24, LANES), F32),
        pltpu.VMEM((3, 4, 4, 8, LANES), F32),
        pltpu.VMEM((3, 4, 4, 8, LANES), F32),
        pltpu.VMEM((4, 8, LANES), F32),
        pltpu.VMEM((4, 8, LANES), F32),
        pltpu.VMEM((32, LANES), F32),
        pltpu.VMEM((32, LANES), F32),
        pltpu.VMEM((3, LANES, LANES), F32),
        pltpu.VMEM((LANES, LANES), F32),
        pltpu.VMEM((3, LANES, LANES), F32),
        pltpu.VMEM((4, 27, 256, 256), BF16),
        pltpu.VMEM((3, 16, 96, 256), BF16),
        pltpu.VMEM((4, 32, LANES), F32),
        pltpu.VMEM((11, 8, LANES), F32),
        dma((6,)),
        dma((SEMS,)),
        dma((SEMS,)),
    ]
    induced, change = pl.pallas_call(
        lambda *refs: kernel(sizes, *refs),
        out_shape=(
            jax.ShapeDtypeStruct((24, LANES), F32),
            jax.ShapeDtypeStruct((1, LANES), F32),
        ),
        in_specs=[hbm] * 6,
        out_specs=(vmem, vmem),
        scratch_shapes=scratch + line_bufs,
        compiler_params=pltpu.CompilerParams(
            collective_id=0, has_side_effects=True, vmem_limit_bytes=VMEM_BYTES
        ),
    )(
        in_hbm(fractions.reshape(3, 4, LANES)),
        in_hbm(polarizability.reshape(4, LANES)),
        in_hbm(occupancy.reshape(4, LANES)),
        in_hbm(pair_mask.reshape(4, 27)),
        in_hbm(perm_field.reshape(24, LANES)),
        in_hbm(history.reshape(6, 24, LANES)),
    )
    return induced.reshape(6, 1, 2, 2, LANES), change[0, 0]


def solution(mesh):
    sizes = {axis: mesh.shape[axis] for axis in AXES}
    placed = (
        P(None, "gx", "gy", "gz", None),
        P("gx", "gy", "gz", None),
        P("gx", "gy", "gz", None),
        P("gx", "gy", "gz", None),
        P(None, "gx", "gy", "gz", None),
        P(None, None, "gx", "gy", "gz", None),
    )
    return jax.shard_map(
        lambda *args: on_device(sizes, *args),
        mesh=mesh,
        in_specs=placed,
        out_specs=(P(None, "gx", "gy", "gz", None), P()),
        check_vma=False,
    )
```

```python
import math

import jax
import jax.numpy as jnp
from jax import lax
from jax.experimental import pallas as pl
from jax.experimental.pallas import tpu as pltpu
from jax.sharding import PartitionSpec as P

AXES = ("gx", "gy", "gz")
FIRST_GROUPS = (("gy",), ("gx",), ("gz",))
LAST_GROUPS = (("gx",), ("gy", "gz"))
MESH = pl.DeviceIdType.MESH
F32 = jnp.float32
BF16 = jnp.bfloat16
LANES = 128
DIRECTIONS = [
    (dx, dy, dz)
    for dx in (-1, 0, 1)
    for dy in (-1, 0, 1)
    for dz in (-1, 0, 1)
    if (dx, dy, dz) != (0, 0, 0)
]
CELL_EDGE = 10.0
SOFTENING = 0.3
THOLE_DAMP = 0.39
RELAXATION = 0.7
LN2 = math.log(2.0)
DAMP_ROOT = math.sqrt(THOLE_DAMP / LN2)
RECEIVERS = [(ry, rz) for ry in (0, 1) for rz in (0, 1)]


SEMS = 8 + len(FIRST_GROUPS) + len(LAST_GROUPS)
VMEM_BYTES = 40 * 1024 * 1024


def away(sizes, axis, step):
    return lax.rem(lax.axis_index(axis) + (step + sizes[axis]), sizes[axis])


def neighbour(sizes, direction):
    return {axis: away(sizes, axis, step) for axis, step in zip(AXES, direction) if step != 0}


def sent_part(step):
    return {0: pl.ds(1, 2), 1: pl.ds(2, 1), -1: pl.ds(1, 1)}[step]


def landing_part(step):
    return {0: pl.ds(1, 2), 1: pl.ds(0, 1), -1: pl.ds(3, 1)}[step]


def remote(src, dst, sems, device):
    return pltpu.make_async_remote_copy(
        src_ref=src,
        dst_ref=dst,
        send_sem=sems[0],
        recv_sem=sems[1],
        device_id=device,
        device_id_type=MESH,
    )


class Batch:
    def __init__(self, copies, counted, sems, device):
        self.copies = copies
        self.whole = remote(counted, counted, sems, device)

    def start(self):
        for copy in self.copies:
            copy.start()

    def arrived(self):
        self.whole.wait_recv()

    def sent(self):
        self.whole.wait_send()


def halo_batch(sizes, buf, sems, same_slab):
    copies = []
    for direction in DIRECTIONS:
        dx, dy, dz = direction
        if (dx == 0) != same_slab:
            continue
        copies.append(
            remote(
                buf.at[pl.ds(1, 1), sent_part(dy), sent_part(dz)],
                buf.at[pl.ds(1 - dx, 1), landing_part(dy), landing_part(dz)],
                sems,
                neighbour(sizes, direction),
            )
        )
    counted = buf.at[1, pl.ds(0, 3)] if same_slab else buf.at[pl.ds(0, 2)]
    return Batch(copies, counted, sems, neighbour(sizes, (0, 0, 1)))


def tile_batch(sizes, buf, sems, tile, counted):
    ry, rz = RECEIVERS[tile]
    mine = buf.at[1, 1 + ry, 1 + rz]
    copies = []
    for dx in (-1, 0, 1):
        for dy, at_y in ((0, 1 + ry), (2 * ry - 1, 3 - 3 * ry)):
            for dz, at_z in ((0, 1 + rz), (2 * rz - 1, 3 - 3 * rz)):
                if (dx, dy, dz) != (0, 0, 0):
                    copies.append(
                        remote(
                            mine,
                            buf.at[1 - dx, at_y, at_z],
                            sems,
                            neighbour(sizes, (dx, dy, dz)),
                        )
                    )
    return Batch(copies, counted, sems, neighbour(sizes, (0, 0, 1)))


def group_steps(sizes, axes):
    steps = [()]
    for axis in axes:
        steps = [step + (n,) for step in steps for n in range(sizes[axis])]
    far = lambda step: sum(min(n, sizes[axis] - n) for n, axis in zip(step, axes))
    return sorted([step for step in steps if any(step)], key=far, reverse=True)


def group_batch(sizes, axes, buf, sems):
    me = 0
    for axis in axes:
        me = me * sizes[axis] + lax.axis_index(axis)
    copies = []
    for step in group_steps(sizes, axes):
        device = {axis: away(sizes, axis, n) for axis, n in zip(axes, step) if n != 0}
        copies.append(remote(buf.at[me], buf.at[me], sems, device))
    counted = buf.at[pl.ds(0, len(copies))]
    return me, Batch(copies, counted, sems, {axes[0]: away(sizes, axes[0], 1)})


def kernel(
    sizes,
    frac_hbm,
    pol_hbm,
    occ_hbm,
    mask_hbm,
    perm_hbm,
    hist_hbm,
    out_ref,
    change_ref,
    frac_ref,
    pol_ref,
    occ_ref,
    mask_ref,
    perm_ref,
    hist_ref,
    own_geo,
    geo,
    past,
    masked,
    moved_one,
    moved_two,
    perm_tiles,
    scaled_tiles,
    receiver,
    own_ends,
    ends,
    own_columns,
    columns,
    pairs,
    feats,
    partial,
    counted,
    in_sems,
    send_sems,
    recv_sems,
    *lines,
):
    lines_one, lines_two = lines[: len(FIRST_GROUPS)], lines[len(FIRST_GROUPS) :]
    sems = [(send_sems.at[n], recv_sems.at[n]) for n in range(SEMS)]

    loads = [
        pltpu.make_async_copy(src, dst, in_sems.at[n])
        for n, (src, dst) in enumerate(
            (
                (frac_hbm, frac_ref),
                (pol_hbm, pol_ref),
                (occ_hbm, occ_ref),
                (hist_hbm, hist_ref),
                (mask_hbm, mask_ref),
                (perm_hbm, perm_ref),
            )
        )
    ]
    for load in loads:
        load.start()

    barrier = pltpu.get_barrier_semaphore()
    greeted = []
    for axis in ("gz", "gx", "gy"):
        greeted += [
            {axis: away(sizes, axis, step)}
            for (step,) in group_steps(sizes, (axis,))
            if 2 <= step <= sizes[axis] - 2
        ]
    greeted += [neighbour(sizes, direction) for direction in DIRECTIONS]
    for device in greeted:
        pl.semaphore_signal(barrier, inc=1, device_id=device, device_id_type=MESH)

    lane = lax.broadcasted_iota(jnp.int32, (1, LANES), 1)
    sub = lax.broadcasted_iota(jnp.int32, (8, LANES), 0)
    lane16 = lax.broadcasted_iota(jnp.int32, (16, LANES), 1)
    sub16 = lax.broadcasted_iota(jnp.int32, (16, LANES), 0)

    loads[0].wait()
    loads[1].wait()
    for tile, (ry, rz) in enumerate(RECEIVERS):
        for which in range(2):
            for c in range(3):
                own_geo[tile, pl.ds(4 * which + c, 1)] = frac_ref[c, pl.ds(tile, 1), :]
            own_geo[tile, pl.ds(4 * which + 3, 1)] = pol_ref[pl.ds(tile, 1), :]
        geo[1, 1 + ry, 1 + rz] = own_geo[tile]

    def positions(slab, rows, sx, tile_y, tile_z):
        kind = lax.rem(rows, 4)
        shift = jnp.where(
            kind == 0,
            jnp.float32(sx - 1.5),
            jnp.where(kind == 1, (tile_y - 2).astype(F32), (tile_z - 2).astype(F32)),
        )
        at = (slab + shift) * CELL_EDGE
        return kind == 3, at, DAMP_ROOT * lax.rsqrt(slab)

    def squared(ref, first):
        parts = [ref[pl.ds(first + n, 1), :] for n in range(3)]
        return parts[0] * parts[0] + parts[1] * parts[1] + parts[2] * parts[2]

    row32 = lax.broadcasted_iota(jnp.int32, (32, LANES), 0)
    last, at, root = positions(
        own_geo[...].reshape(32, LANES), row32, 1, 1 + row32 // 16, 1 + lax.rem(row32 // 8, 2)
    )
    receiver[...] = jnp.where(last, -root, 2.0 * at)
    own_ends[...] = jnp.where(last, root, at)
    for tile in range(4):
        square = squared(own_ends, 8 * tile)
        receiver[pl.ds(8 * tile + 4, 1)] = square + SOFTENING
        own_ends[pl.ds(8 * tile + 4, 1)] = square
    own_columns[...] = jnp.transpose(
        jnp.concatenate([own_ends[...], jnp.zeros((96, LANES), F32)], axis=0)
    )

    def pair_factors(cols, places, offset_of, sx, first):
        for at, sy, sz in places:
            source = [
                jnp.broadcast_to(cols[:, at + n : at + n + 1], (16, LANES)) for n in range(5)
            ]
            for tile, (ry, rz) in enumerate(RECEIVERS):
                ky, kz = sy - ry, sz - rz
                if not (0 <= ky <= 2 and 0 <= kz <= 2):
                    continue
                damp = source[3] * receiver[pl.ds(8 * tile + 3, 1), :]
                dist = source[4] + receiver[pl.ds(8 * tile + 4, 1), :]
                for n in range(3):
                    dist = dist - source[n] * receiver[pl.ds(8 * tile + n, 1), :]
                offset = 9 * sx + 3 * ky + kz
                allowed = 3.0 * mask_ref[tile, offset].astype(F32)
                root = lax.rsqrt(dist)
                inverse = root * root
                cube = root * inverse * allowed
                if offset_of == "own" and ky == 1 and kz == 1:
                    cube = jnp.where(sub16 + first != lane16, cube, 0.0)
                power = dist * dist * root * damp
                fade = jnp.exp2(power)
                three = 1.0 - fade
                five = three + (power * LN2) * fade
                for part, value in ((0, five * (inverse * cube)), (128, three * cube)):
                    high = value.astype(BF16)
                    low = (value - high.astype(F32)).astype(BF16)
                    rows = pl.ds(pl.multiple_of(first + part, 16), 16)
                    pairs[tile, offset, rows, pl.ds(0, 128)] = high
                    pairs[tile, offset, rows, pl.ds(128, 128)] = low

    loads[2].wait()
    loads[3].wait()
    filled = occ_ref[...].astype(F32)
    filled_rows = jnp.concatenate([filled] * 6, axis=0)
    for h in range(6):
        masked[h] = hist_ref[h] * filled_rows
    row = jnp.zeros((1, LANES), F32)
    for a in range(6):
        for b in range(a, 6):
            product = masked[a] * masked[b]
            folded = product[0:8] + product[8:16] + product[16:24]
            value = jnp.sum(jnp.sum(folded, axis=0, keepdims=True), axis=1, keepdims=True)
            row = jnp.where(lane == 6 * a + b, value, row)

    for tile, (ry, rz) in enumerate(RECEIVERS):
        own = (1, 1 + ry, 1 + rz)
        for h in range(5):
            past[own + (pl.ds(6 * h, 6),)] = masked[h + 1, pl.ds(tile, 6, stride=4), :]
        past[own + (pl.ds(30, 2),)] = jnp.zeros((2, LANES), F32)

    own_places = [(8 * tile, 1 + ry, 1 + rz) for tile, (ry, rz) in enumerate(RECEIVERS)]
    all_places = [(8 * (4 * sy + sz), sy, sz) for sy in range(4) for sz in range(4)]
    rim_places = [(at, sy, sz) for at, sy, sz in all_places if sy in (0, 3) or sz in (0, 3)]

    def own_block(block, carry):
        for part in range(4):
            first = pl.multiple_of(block * 64 + part * 16, 16)
            pair_factors(own_columns[pl.ds(first, 16), :], own_places, "own", 1, first)
        return carry

    def clear(number, carry):
        sx, s = number // 16, lax.rem(number, 16)
        for piece in range(3):
            feats[sx, s, pl.ds(32 * piece, 16), pl.ds(128, 128)] = jnp.zeros((16, LANES), BF16)
        return carry

    def send_group(groups, number, bufs, first_sem, values):
        me, batch = group_batch(sizes, groups[number], bufs[number], sems[first_sem + number])
        bufs[number][me] = values
        batch.start()
        return batch

    def total(bufs, number, batch):
        batch.arrived()
        return jnp.sum(bufs[number][...], axis=0)

    pl.semaphore_wait(barrier, len(greeted))

    geo_batches = [halo_batch(sizes, geo, sems[n], n == 0) for n in range(2)]
    past_batches = [
        halo_batch(sizes, past, sems[2], True),
        Batch(
            [
                remote(past.at[1], past.at[1 - dx], sems[3], neighbour(sizes, (dx, 0, 0)))
                for dx in (-1, 1)
            ],
            past.at[pl.ds(0, 2)],
            sems[3],
            neighbour(sizes, (1, 0, 0)),
        ),
    ]
    line_a = send_group(FIRST_GROUPS, 0, lines_one, 8, row)
    for batch in geo_batches:
        batch.start()
    past_batches[0].start()

    loads[4].wait()
    lax.fori_loop(0, 2, own_block, 0)

    row = total(lines_one, 0, line_a)
    line_b = send_group(FIRST_GROUPS, 1, lines_one, 8, row)

    lax.fori_loop(0, 48, clear, 0, unroll=4)
    loads[5].wait()
    for tile in range(4):
        weight = jnp.broadcast_to(
            RELAXATION * occ_ref[pl.ds(tile, 1), :].astype(F32) * pol_ref[pl.ds(tile, 1), :],
            (8, LANES),
        )
        scaled_tiles[tile] = jnp.where(lax.rem(sub, 4) == 3, 0.0, weight)
        perm_tiles[tile] = jnp.zeros((8, LANES), F32)
        for which in range(2):
            perm_tiles[tile, pl.ds(4 * which, 3), :] = perm_ref[
                pl.ds(12 * which + tile, 3, stride=4), :
            ]

    row128 = lax.broadcasted_iota(jnp.int32, (LANES, LANES), 0)

    def place_slab(sx):
        last, at, root = positions(
            geo[sx].reshape(LANES, LANES), row128, sx, row128 // 32, lax.rem(row128 // 8, 4)
        )
        ends[sx] = jnp.where(last, 1.0, at)
        lengths = at * at
        lengths = (
            lengths
            + pltpu.roll(lengths, LANES - 1, 0)
            + pltpu.roll(lengths, LANES - 2, 0)
        )
        columns[sx] = jnp.transpose(
            jnp.where(lax.rem(row128, 8) == 4, lengths, jnp.where(last, root, at))
        )

    geo_batches[0].arrived()
    place_slab(1)

    def rim_block(block, carry):
        for part in range(4):
            first = pl.multiple_of(block * 64 + part * 16, 16)
            pair_factors(columns[1, pl.ds(first, 16), :], rim_places, "rim", 1, first)
        return carry

    lax.fori_loop(0, 2, rim_block, 0)

    past_batches[0].arrived()
    past_batches[1].start()
    geo_batches[1].arrived()
    place_slab(0)
    place_slab(2)

    def side_block(step, carry):
        sx = 2 * (step // 2)
        for part in range(4):
            first = pl.multiple_of(lax.rem(step, 2) * 64 + part * 16, 16)
            pair_factors(columns[sx, pl.ds(first, 16), :], all_places, "side", sx, first)
        return carry

    lax.fori_loop(0, 1, side_block, 0)
    row = total(lines_one, 1, line_b)
    line_c = send_group(FIRST_GROUPS, 2, lines_one, 8, row)
    lax.fori_loop(1, 4, side_block, 0)
    row = total(lines_one, 2, line_c)

    def entry(a, b):
        return jnp.sum(
            jnp.where(lane == 6 * min(a, b) + max(a, b), row, 0.0), axis=1, keepdims=True
        )

    gram = {(a, b): entry(a, b) for a in range(6) for b in range(a, 6) if a < 5}
    trace = gram[0, 0] + gram[1, 1] + gram[2, 2] + gram[3, 3] + gram[4, 4]
    ridge = 0.001 * trace / 5.0 + 1.0
    low = {}
    scale = []
    half = []
    for a in range(5):
        pivot = gram[a, a] + ridge
        for c in range(a):
            pivot = pivot - low[a, c] * low[a, c]
        scale.append(lax.rsqrt(pivot))
        for b in range(a + 1, 5):
            value = gram[a, b]
            for c in range(a):
                value = value - low[a, c] * low[b, c]
            low[b, a] = value * scale[a]
        value = gram[a, 5]
        for c in range(a):
            value = value - low[a, c] * half[c]
        half.append(value * scale[a])
    coeffs = [None] * 5
    for a in reversed(range(5)):
        value = half[a]
        for b in range(a + 1, 5):
            value = value - low[b, a] * coeffs[b]
        coeffs[a] = value * scale[a]
    coeffs = [jnp.broadcast_to(value, (8, LANES))[0:6] for value in coeffs]

    past_batches[1].arrived()

    first_set = sub < 4
    flat = jnp.zeros((8, LANES), F32)

    def write_feats(sx, s, tile_ref):
        whole = tile_ref[...]
        near = ends[sx, pl.ds(8 * s, 8), :]
        multipliers = []
        along = None
        for b in range(3):
            both = jnp.where(first_set, whole[b : b + 1], whole[4 + b : 5 + b])
            multipliers.append(both)
            term = near[b : b + 1] * both
            along = term if along is None else along + term
        multipliers.append(along)
        parts = [near * value for value in multipliers]
        for half_at in range(2):
            value = jnp.concatenate(parts[2 * half_at : 2 * half_at + 2], axis=0)
            for piece in range(3):
                kept = value.astype(BF16)
                feats[sx, s, pl.ds(32 * piece + 16 * half_at, 16), pl.ds(0, 128)] = kept
                value = value - kept.astype(F32)
        value = jnp.concatenate([flat, whole * (-1.0 / 3.0)], axis=0)
        for piece in range(3):
            kept = value.astype(BF16)
            feats[sx, s, pl.ds(32 * piece + 16, 16), pl.ds(128, 128)] = kept
            value = value - kept.astype(F32)

    def predict(sx, carry):
        for s in range(16):
            sy, sz = s // 4, s % 4
            value = None
            for h in range(5):
                term = coeffs[h] * past[sx, sy, sz, pl.ds(6 * h, 6), :]
                value = term if value is None else value + term
            moved_one[sx, sy, sz] = flat
            moved_one[sx, sy, sz, pl.ds(0, 3), :] = value[0:3]
            moved_one[sx, sy, sz, pl.ds(4, 3), :] = value[3:6]
        for s in range(16):
            write_feats(sx, s, moved_one.at[sx, s // 4, s % 4])
        return carry

    lax.fori_loop(0, 3, predict, 0)

    def dot_part(tile, sources):
        if len(sources) > 6:
            middle = len(sources) // 2
            return dot_piece(tile, sources[:middle]) + dot_piece(tile, sources[middle:])
        return dot_piece(tile, sources)

    def joined(summed):
        both = summed[:, 0:128] + summed[:, 128:256]
        return both[0:32] + both[32:64] + both[64:96]

    def dot_piece(tile, sources):
        ry, rz = RECEIVERS[tile]
        lhs = jnp.concatenate([feats[sx, 4 * sy + sz] for sx, sy, sz in sources], axis=1)
        rhs = jnp.concatenate(
            [pairs[tile, 9 * sx + 3 * (sy - ry) + sz - rz] for sx, sy, sz in sources], axis=0
        )
        return joined(jnp.dot(lhs, rhs, preferred_element_type=F32))

    def sources_of(tile, wanted=lambda source: True):
        ry, rz = RECEIVERS[tile]
        sources = [
            (sx, ry + ky, rz + kz) for sx in range(3) for ky in range(3) for kz in range(3)
        ]
        return [source for source in sources if wanted(source)]

    def relaxed(tile, before, out):
        ry, rz = RECEIVERS[tile]
        here = ends[1, pl.ds(8 * (4 * (ry + 1) + rz + 1), 8), :]
        value = out[24:32]
        for b in range(3):
            value = value - here[b : b + 1] * out[8 * b : 8 * b + 8]
        shared = jnp.where(first_set, value[3:4], value[7:8])
        field = value - here * shared
        return (1.0 - RELAXATION) * before + scaled_tiles[tile] * (perm_tiles[tile] + field)

    tile_batches = []
    summed = dot_part(0, sources_of(0))
    for tile, (ry, rz) in enumerate(RECEIVERS):
        now = summed
        if tile < 3:
            summed = dot_part(tile + 1, sources_of(tile + 1))
        before = moved_one[1, 1 + ry, 1 + rz]
        moved_two[1, 1 + ry, 1 + rz] = relaxed(tile, before, now)
        tile_batches.append(tile_batch(sizes, moved_two, sems[4 + tile], tile, counted))
        tile_batches[-1].start()

    for batch in geo_batches + past_batches + [line_a, line_b, line_c]:
        batch.sent()

    own_sources = [(1, 1 + ry, 1 + rz) for ry, rz in RECEIVERS]

    def kind_of(source):
        return 2 * ((source[1] + 1) % 2) + (source[2] + 1) % 2

    for sx, sy, sz in own_sources:
        write_feats(sx, 4 * sy + sz, moved_two.at[sx, sy, sz])
    for tile in range(4):
        partial[tile] = dot_part(tile, own_sources)

    changed = flat
    size = flat
    for kinds in ((0, 1), (2, 3)):
        for kind in kinds:
            tile_batches[kind].arrived()

        def arriving(source):
            return kind_of(source) in kinds and source not in own_sources

        for source in [(sx, sy, sz) for sx in range(3) for sy in range(4) for sz in range(4)]:
            if arriving(source):
                sx, sy, sz = source
                write_feats(sx, 4 * sy + sz, moved_two.at[sx, sy, sz])
        for tile, (ry, rz) in enumerate(RECEIVERS):
            summed = partial[tile] + dot_part(tile, sources_of(tile, arriving))
            if kinds[-1] < 3:
                partial[tile] = summed
                continue
            before = moved_two[1, 1 + ry, 1 + rz]
            after = relaxed(tile, before, summed)
            out_ref[pl.ds(tile, 3, stride=4), :] = after[0:3]
            out_ref[pl.ds(12 + tile, 3, stride=4), :] = after[4:7]
            update = after - before
            changed = changed + update * update
            size = size + after * after

    def whole_sum(value):
        return jnp.sum(jnp.sum(value, axis=0, keepdims=True), axis=1, keepdims=True)

    row = jnp.where(lane == 0, whole_sum(changed), jnp.where(lane == 1, whole_sum(size), 0.0))
    ending = []
    for number in range(len(LAST_GROUPS)):
        ending.append(send_group(LAST_GROUPS, number, lines_two, 8 + len(FIRST_GROUPS), row))
        if number == 0:
            for batch in tile_batches:
                batch.sent()
        row = total(lines_two, number, ending[-1])
    top = jnp.sum(jnp.where(lane == 0, row, 0.0), axis=1, keepdims=True)
    bottom = jnp.sum(jnp.where(lane == 1, row, 0.0), axis=1, keepdims=True)
    change_ref[...] = jnp.broadcast_to(jnp.sqrt(top / (bottom + 1.0)), (1, LANES))

    for batch in ending:
        batch.sent()


def in_hbm(array):
    return pltpu.with_memory_space_constraint(array, pltpu.HBM)


def on_device(sizes, fractions, polarizability, occupancy, pair_mask, perm_field, history):
    vmem = pl.BlockSpec(memory_space=pltpu.VMEM)
    hbm = pl.BlockSpec(memory_space=pltpu.HBM)
    dma = pltpu.SemaphoreType.DMA
    line_bufs = [
        pltpu.VMEM((math.prod(sizes[axis] for axis in axes), 1, LANES), F32)
        for axes in FIRST_GROUPS + LAST_GROUPS
    ]
    scratch = [
        pltpu.VMEM((3, 4, LANES), F32),
        pltpu.VMEM((4, LANES), F32),
        pltpu.VMEM((4, LANES), jnp.int32),
        pltpu.SMEM((4, 27), jnp.int32),
        pltpu.VMEM((24, LANES), F32),
        pltpu.VMEM((6, 24, LANES), F32),
        pltpu.VMEM((4, 8, LANES), F32),
        pltpu.VMEM((3, 4, 4, 8, LANES), F32),
        pltpu.VMEM((3, 4, 4, 32, LANES), F32),
        pltpu.VMEM((6, 24, LANES), F32),
        pltpu.VMEM((3, 4, 4, 8, LANES), F32),
        pltpu.VMEM((3, 4, 4, 8, LANES), F32),
        pltpu.VMEM((4, 8, LANES), F32),
        pltpu.VMEM((4, 8, LANES), F32),
        pltpu.VMEM((32, LANES), F32),
        pltpu.VMEM((32, LANES), F32),
        pltpu.VMEM((3, LANES, LANES), F32),
        pltpu.VMEM((LANES, LANES), F32),
        pltpu.VMEM((3, LANES, LANES), F32),
        pltpu.VMEM((4, 27, 256, 256), BF16),
        pltpu.VMEM((3, 16, 96, 256), BF16),
        pltpu.VMEM((4, 32, LANES), F32),
        pltpu.VMEM((11, 8, LANES), F32),
        dma((6,)),
        dma((SEMS,)),
        dma((SEMS,)),
    ]
    induced, change = pl.pallas_call(
        lambda *refs: kernel(sizes, *refs),
        out_shape=(
            jax.ShapeDtypeStruct((24, LANES), F32),
            jax.ShapeDtypeStruct((1, LANES), F32),
        ),
        in_specs=[hbm] * 6,
        out_specs=(vmem, vmem),
        scratch_shapes=scratch + line_bufs,
        compiler_params=pltpu.CompilerParams(
            collective_id=0, has_side_effects=True, vmem_limit_bytes=VMEM_BYTES
        ),
    )(
        in_hbm(fractions.reshape(3, 4, LANES)),
        in_hbm(polarizability.reshape(4, LANES)),
        in_hbm(occupancy.reshape(4, LANES)),
        in_hbm(pair_mask.reshape(4, 27)),
        in_hbm(perm_field.reshape(24, LANES)),
        in_hbm(history.reshape(6, 24, LANES)),
    )
    return induced.reshape(6, 1, 2, 2, LANES), change[0, 0]


def solution(mesh):
    sizes = {axis: mesh.shape[axis] for axis in AXES}
    placed = (
        P(None, "gx", "gy", "gz", None),
        P("gx", "gy", "gz", None),
        P("gx", "gy", "gz", None),
        P("gx", "gy", "gz", None),
        P(None, "gx", "gy", "gz", None),
        P(None, None, "gx", "gy", "gz", None),
    )
    return jax.shard_map(
        lambda *args: on_device(sizes, *args),
        mesh=mesh,
        in_specs=placed,
        out_specs=(P(None, "gx", "gy", "gz", None), P()),
        check_vma=False,
    )
```

```python
import math

import jax
import jax.numpy as jnp
from jax import lax
from jax.experimental import pallas as pl
from jax.experimental.pallas import tpu as pltpu
from jax.sharding import PartitionSpec as P

AXES = ("gx", "gy", "gz")
FIRST_GROUPS = (("gy",), ("gx",), ("gz",))
LAST_GROUPS = (("gx",), ("gy", "gz"))
MESH = pl.DeviceIdType.MESH
F32 = jnp.float32
BF16 = jnp.bfloat16
LANES = 128
DIRECTIONS = [
    (dx, dy, dz)
    for dx in (-1, 0, 1)
    for dy in (-1, 0, 1)
    for dz in (-1, 0, 1)
    if (dx, dy, dz) != (0, 0, 0)
]
CELL_EDGE = 10.0
SOFTENING = 0.3
THOLE_DAMP = 0.39
RELAXATION = 0.7
LN2 = math.log(2.0)
DAMP_ROOT = math.sqrt(THOLE_DAMP / LN2)
RECEIVERS = [(ry, rz) for ry in (0, 1) for rz in (0, 1)]


SEMS = 9 + len(FIRST_GROUPS) + len(LAST_GROUPS)
VMEM_BYTES = 40 * 1024 * 1024


def away(sizes, axis, step):
    return lax.rem(lax.axis_index(axis) + (step + sizes[axis]), sizes[axis])


def neighbour(sizes, direction):
    return {axis: away(sizes, axis, step) for axis, step in zip(AXES, direction) if step != 0}


def sent_part(step):
    return {0: pl.ds(1, 2), 1: pl.ds(2, 1), -1: pl.ds(1, 1)}[step]


def landing_part(step):
    return {0: pl.ds(1, 2), 1: pl.ds(0, 1), -1: pl.ds(3, 1)}[step]


def remote(src, dst, sems, device):
    return pltpu.make_async_remote_copy(
        src_ref=src,
        dst_ref=dst,
        send_sem=sems[0],
        recv_sem=sems[1],
        device_id=device,
        device_id_type=MESH,
    )


class Batch:
    def __init__(self, copies, counted, sems, device):
        self.copies = copies
        self.whole = remote(counted, counted, sems, device)

    def start(self):
        for copy in self.copies:
            copy.start()

    def arrived(self):
        self.whole.wait_recv()

    def sent(self):
        self.whole.wait_send()


def halo_copies(sizes, buf, sems, wanted):
    copies = []
    for direction in DIRECTIONS:
        dx, dy, dz = direction
        if wanted(direction):
            copies.append(
                remote(
                    buf.at[pl.ds(1, 1), sent_part(dy), sent_part(dz)],
                    buf.at[pl.ds(1 - dx, 1), landing_part(dy), landing_part(dz)],
                    sems,
                    neighbour(sizes, direction),
                )
            )
    return copies


def slab_batch(sizes, buf, sems):
    copies = halo_copies(sizes, buf, sems, lambda direction: direction[0] == 0)
    return Batch(copies, buf.at[1, pl.ds(0, 3)], sems, neighbour(sizes, (0, 0, 1)))


def chip_batches(sizes, buf, chip_sems, sems, counted):
    odd = lax.rem(lax.axis_index("gx"), 2)
    me = lax.axis_index("gx") + sizes["gx"]
    tiles = (pl.ds(1, 2), pl.ds(1, 2))
    mine = buf.at[(1,) + tiles]
    partner = {"gx": lax.rem(me + 1 - 2 * odd, sizes["gx"])}
    beyond = {"gx": lax.rem(me - 1 + 2 * odd, sizes["gx"])}
    near = Batch(
        [remote(mine, buf.at[(2 * odd,) + tiles], chip_sems, partner)],
        buf.at[0, pl.ds(0, 1)],
        chip_sems,
        partner,
    )
    copies = [remote(mine, buf.at[(2 - 2 * odd,) + tiles], sems, beyond)]
    copies += halo_copies(
        sizes, buf, sems, lambda direction: direction[0] != 0 and any(direction[1:])
    )
    return near, Batch(copies, counted, sems, partner)


def tile_batch(sizes, buf, sems, tile, counted):
    ry, rz = RECEIVERS[tile]
    mine = buf.at[1, 1 + ry, 1 + rz]
    copies = []
    for dx in (-1, 0, 1):
        for dy, at_y in ((0, 1 + ry), (2 * ry - 1, 3 - 3 * ry)):
            for dz, at_z in ((0, 1 + rz), (2 * rz - 1, 3 - 3 * rz)):
                if (dx, dy, dz) != (0, 0, 0):
                    copies.append(
                        remote(
                            mine,
                            buf.at[1 - dx, at_y, at_z],
                            sems,
                            neighbour(sizes, (dx, dy, dz)),
                        )
                    )
    return Batch(copies, counted, sems, neighbour(sizes, (0, 0, 1)))


def group_steps(sizes, axes):
    steps = [()]
    for axis in axes:
        steps = [step + (n,) for step in steps for n in range(sizes[axis])]
    far = lambda step: sum(min(n, sizes[axis] - n) for n, axis in zip(step, axes))
    return sorted([step for step in steps if any(step)], key=far, reverse=True)


def group_batch(sizes, axes, buf, sems):
    me = 0
    for axis in axes:
        me = me * sizes[axis] + lax.axis_index(axis)
    copies = []
    for step in group_steps(sizes, axes):
        device = {axis: away(sizes, axis, n) for axis, n in zip(axes, step) if n != 0}
        copies.append(remote(buf.at[me], buf.at[me], sems, device))
    counted = buf.at[pl.ds(0, len(copies))]
    return me, Batch(copies, counted, sems, {axes[0]: away(sizes, axes[0], 1)})


def kernel(
    sizes,
    frac_hbm,
    pol_hbm,
    occ_hbm,
    mask_hbm,
    perm_hbm,
    hist_hbm,
    out_ref,
    change_ref,
    frac_ref,
    pol_ref,
    occ_ref,
    mask_ref,
    perm_ref,
    hist_ref,
    own_geo,
    geo,
    past,
    masked,
    moved_one,
    moved_two,
    perm_tiles,
    scaled_tiles,
    receiver,
    own_ends,
    ends,
    own_columns,
    near_columns,
    columns,
    pairs,
    feats,
    partial,
    counted,
    in_sems,
    send_sems,
    recv_sems,
    *lines,
):
    lines_one, lines_two = lines[: len(FIRST_GROUPS)], lines[len(FIRST_GROUPS) :]
    sems = [(send_sems.at[n], recv_sems.at[n]) for n in range(SEMS)]

    loads = [
        pltpu.make_async_copy(src, dst, in_sems.at[n])
        for n, (src, dst) in enumerate(
            (
                (frac_hbm, frac_ref),
                (pol_hbm, pol_ref),
                (occ_hbm, occ_ref),
                (hist_hbm, hist_ref),
                (mask_hbm, mask_ref),
                (perm_hbm, perm_ref),
            )
        )
    ]
    for load in loads:
        load.start()

    barrier = pltpu.get_barrier_semaphore()
    greeted = []
    for axis in ("gz", "gx", "gy"):
        greeted += [
            {axis: away(sizes, axis, step)}
            for (step,) in group_steps(sizes, (axis,))
            if 2 <= step <= sizes[axis] - 2
        ]
    greeted += [neighbour(sizes, direction) for direction in DIRECTIONS]
    for device in greeted:
        pl.semaphore_signal(barrier, inc=1, device_id=device, device_id_type=MESH)

    lane = lax.broadcasted_iota(jnp.int32, (1, LANES), 1)
    sub = lax.broadcasted_iota(jnp.int32, (8, LANES), 0)
    lane16 = lax.broadcasted_iota(jnp.int32, (16, LANES), 1)
    sub16 = lax.broadcasted_iota(jnp.int32, (16, LANES), 0)

    loads[0].wait()
    loads[1].wait()
    for tile, (ry, rz) in enumerate(RECEIVERS):
        for which in range(2):
            for c in range(3):
                own_geo[tile, pl.ds(4 * which + c, 1)] = frac_ref[c, pl.ds(tile, 1), :]
            own_geo[tile, pl.ds(4 * which + 3, 1)] = pol_ref[pl.ds(tile, 1), :]
        geo[1, 1 + ry, 1 + rz] = own_geo[tile]

    def positions(slab, rows, sx, tile_y, tile_z):
        sx = jnp.asarray(sx).astype(F32)
        kind = lax.rem(rows, 4)
        shift = jnp.where(
            kind == 0,
            sx - 1.5,
            jnp.where(kind == 1, (tile_y - 2).astype(F32), (tile_z - 2).astype(F32)),
        )
        at = (slab + shift) * CELL_EDGE
        return kind == 3, at, DAMP_ROOT * lax.rsqrt(slab)

    def squared(ref, first):
        parts = [ref[pl.ds(first + n, 1), :] for n in range(3)]
        return parts[0] * parts[0] + parts[1] * parts[1] + parts[2] * parts[2]

    row32 = lax.broadcasted_iota(jnp.int32, (32, LANES), 0)
    last, at, root = positions(
        own_geo[...].reshape(32, LANES), row32, 1, 1 + row32 // 16, 1 + lax.rem(row32 // 8, 2)
    )
    receiver[...] = jnp.where(last, -root, 2.0 * at)
    own_ends[...] = jnp.where(last, root, at)
    for tile in range(4):
        square = squared(own_ends, 8 * tile)
        receiver[pl.ds(8 * tile + 4, 1)] = square + SOFTENING
        own_ends[pl.ds(8 * tile + 4, 1)] = square
    own_columns[...] = jnp.transpose(
        jnp.concatenate([own_ends[...], jnp.zeros((96, LANES), F32)], axis=0)
    )

    def pair_factors(cols, places, offset_of, sx, first):
        for at, sy, sz in places:
            source = [
                jnp.broadcast_to(cols[:, at + n : at + n + 1], (16, LANES)) for n in range(5)
            ]
            for tile, (ry, rz) in enumerate(RECEIVERS):
                ky, kz = sy - ry, sz - rz
                if not (0 <= ky <= 2 and 0 <= kz <= 2):
                    continue
                damp = source[3] * receiver[pl.ds(8 * tile + 3, 1), :]
                dist = source[4] + receiver[pl.ds(8 * tile + 4, 1), :]
                for n in range(3):
                    dist = dist - source[n] * receiver[pl.ds(8 * tile + n, 1), :]
                offset = 9 * sx + 3 * ky + kz
                allowed = 3.0 * mask_ref[tile, offset].astype(F32)
                root = lax.rsqrt(dist)
                inverse = root * root
                cube = root * inverse * allowed
                if offset_of == "own" and ky == 1 and kz == 1:
                    cube = jnp.where(sub16 + first != lane16, cube, 0.0)
                power = dist * dist * root * damp
                fade = jnp.exp2(power)
                three = 1.0 - fade
                five = three + (power * LN2) * fade
                for part, value in ((0, five * (inverse * cube)), (128, three * cube)):
                    high = value.astype(BF16)
                    low = (value - high.astype(F32)).astype(BF16)
                    rows = pl.ds(pl.multiple_of(first + part, 16), 16)
                    pairs[tile, offset, rows, pl.ds(0, 128)] = high
                    pairs[tile, offset, rows, pl.ds(128, 128)] = low

    loads[2].wait()
    loads[3].wait()
    filled = occ_ref[...].astype(F32)
    filled_rows = jnp.concatenate([filled] * 6, axis=0)
    for h in range(6):
        masked[h] = hist_ref[h] * filled_rows
    row = jnp.zeros((1, LANES), F32)
    for a in range(6):
        for b in range(a, 6):
            product = masked[a] * masked[b]
            folded = product[0:8] + product[8:16] + product[16:24]
            value = jnp.sum(jnp.sum(folded, axis=0, keepdims=True), axis=1, keepdims=True)
            row = jnp.where(lane == 6 * a + b, value, row)

    for tile, (ry, rz) in enumerate(RECEIVERS):
        own = (1, 1 + ry, 1 + rz)
        for h in range(5):
            past[own + (pl.ds(6 * h, 6),)] = masked[h + 1, pl.ds(tile, 6, stride=4), :]
        past[own + (pl.ds(30, 2),)] = jnp.zeros((2, LANES), F32)

    own_places = [(8 * tile, 1 + ry, 1 + rz) for tile, (ry, rz) in enumerate(RECEIVERS)]
    all_places = [(8 * (4 * sy + sz), sy, sz) for sy in range(4) for sz in range(4)]
    rim_places = [(at, sy, sz) for at, sy, sz in all_places if sy in (0, 3) or sz in (0, 3)]

    def own_block(block, carry):
        for part in range(4):
            first = pl.multiple_of(block * 64 + part * 16, 16)
            pair_factors(own_columns[pl.ds(first, 16), :], own_places, "own", 1, first)
        return carry

    def clear(number, carry):
        sx, s = number // 16, lax.rem(number, 16)
        for piece in range(3):
            feats[sx, s, pl.ds(32 * piece, 16), pl.ds(128, 128)] = jnp.zeros((16, LANES), BF16)
        return carry

    def send_group(groups, number, bufs, first_sem, values):
        me, batch = group_batch(sizes, groups[number], bufs[number], sems[first_sem + number])
        bufs[number][me] = values
        batch.start()
        return batch

    def total(bufs, number, batch):
        batch.arrived()
        return jnp.sum(bufs[number][...], axis=0)

    pl.semaphore_wait(barrier, len(greeted))

    near_batch, far_batch = chip_batches(sizes, geo, sems[SEMS - 1], sems[1], counted)
    geo_batches = [near_batch, slab_batch(sizes, geo, sems[0]), far_batch]
    past_batches = [
        slab_batch(sizes, past, sems[2]),
        Batch(
            [
                remote(past.at[1], past.at[1 - dx], sems[3], neighbour(sizes, (dx, 0, 0)))
                for dx in (-1, 1)
            ],
            past.at[pl.ds(0, 2)],
            sems[3],
            neighbour(sizes, (1, 0, 0)),
        ),
    ]
    line_a = send_group(FIRST_GROUPS, 0, lines_one, 8, row)
    for batch in geo_batches:
        batch.start()
    past_batches[0].start()

    loads[4].wait()
    lax.fori_loop(0, 2, own_block, 0)

    odd = lax.rem(lax.axis_index("gx"), 2)
    near_slab, far_slab = 2 - 2 * odd, 2 * odd

    near_batch.arrived()
    last, at, root = positions(
        geo[near_slab, pl.ds(1, 2), pl.ds(1, 2)].reshape(32, LANES),
        row32,
        near_slab,
        1 + row32 // 16,
        1 + lax.rem(row32 // 8, 2),
    )
    lengths = at * at
    lengths = lengths + pltpu.roll(lengths, 31, 0) + pltpu.roll(lengths, 30, 0)
    near_columns[...] = jnp.transpose(
        jnp.concatenate(
            [
                jnp.where(lax.rem(row32, 8) == 4, lengths, jnp.where(last, root, at)),
                jnp.zeros((96, LANES), F32),
            ],
            axis=0,
        )
    )

    def near_block(block, carry):
        for part in range(4):
            first = pl.multiple_of(block * 64 + part * 16, 16)
            pair_factors(near_columns[pl.ds(first, 16), :], own_places, "near", near_slab, first)
        return carry

    lax.fori_loop(0, 2, near_block, 0)

    row = total(lines_one, 0, line_a)
    line_b = send_group(FIRST_GROUPS, 1, lines_one, 8, row)

    lax.fori_loop(0, 48, clear, 0, unroll=4)
    loads[5].wait()
    for tile in range(4):
        weight = jnp.broadcast_to(
            RELAXATION * occ_ref[pl.ds(tile, 1), :].astype(F32) * pol_ref[pl.ds(tile, 1), :],
            (8, LANES),
        )
        scaled_tiles[tile] = jnp.where(lax.rem(sub, 4) == 3, 0.0, weight)
        perm_tiles[tile] = jnp.zeros((8, LANES), F32)
        for which in range(2):
            perm_tiles[tile, pl.ds(4 * which, 3), :] = perm_ref[
                pl.ds(12 * which + tile, 3, stride=4), :
            ]

    row128 = lax.broadcasted_iota(jnp.int32, (LANES, LANES), 0)

    def place_slab(sx):
        last, at, root = positions(
            geo[sx].reshape(LANES, LANES), row128, sx, row128 // 32, lax.rem(row128 // 8, 4)
        )
        ends[sx] = jnp.where(last, 1.0, at)
        lengths = at * at
        lengths = (
            lengths
            + pltpu.roll(lengths, LANES - 1, 0)
            + pltpu.roll(lengths, LANES - 2, 0)
        )
        columns[sx] = jnp.transpose(
            jnp.where(lax.rem(row128, 8) == 4, lengths, jnp.where(last, root, at))
        )

    geo_batches[1].arrived()
    place_slab(1)

    def rim_block(block, carry):
        for part in range(4):
            first = pl.multiple_of(block * 64 + part * 16, 16)
            pair_factors(columns[1, pl.ds(first, 16), :], rim_places, "rim", 1, first)
        return carry

    lax.fori_loop(0, 2, rim_block, 0)

    past_batches[0].arrived()
    past_batches[1].start()
    geo_batches[2].arrived()
    place_slab(0)
    place_slab(2)

    def near_rim_block(block, carry):
        for part in range(4):
            first = pl.multiple_of(block * 64 + part * 16, 16)
            cols = columns[near_slab, pl.ds(first, 16), :]
            pair_factors(cols, rim_places, "near", near_slab, first)
        return carry

    def far_block(block, carry):
        for part in range(4):
            first = pl.multiple_of(block * 64 + part * 16, 16)
            pair_factors(columns[far_slab, pl.ds(first, 16), :], all_places, "far", far_slab, first)
        return carry

    lax.fori_loop(0, 1, near_rim_block, 0)
    row = total(lines_one, 1, line_b)
    line_c = send_group(FIRST_GROUPS, 2, lines_one, 8, row)
    lax.fori_loop(1, 2, near_rim_block, 0)
    lax.fori_loop(0, 2, far_block, 0)
    row = total(lines_one, 2, line_c)

    def entry(a, b):
        return jnp.sum(
            jnp.where(lane == 6 * min(a, b) + max(a, b), row, 0.0), axis=1, keepdims=True
        )

    gram = {(a, b): entry(a, b) for a in range(6) for b in range(a, 6) if a < 5}
    trace = gram[0, 0] + gram[1, 1] + gram[2, 2] + gram[3, 3] + gram[4, 4]
    ridge = 0.001 * trace / 5.0 + 1.0
    low = {}
    scale = []
    half = []
    for a in range(5):
        pivot = gram[a, a] + ridge
        for c in range(a):
            pivot = pivot - low[a, c] * low[a, c]
        scale.append(lax.rsqrt(pivot))
        for b in range(a + 1, 5):
            value = gram[a, b]
            for c in range(a):
                value = value - low[a, c] * low[b, c]
            low[b, a] = value * scale[a]
        value = gram[a, 5]
        for c in range(a):
            value = value - low[a, c] * half[c]
        half.append(value * scale[a])
    coeffs = [None] * 5
    for a in reversed(range(5)):
        value = half[a]
        for b in range(a + 1, 5):
            value = value - low[b, a] * coeffs[b]
        coeffs[a] = value * scale[a]
    coeffs = [jnp.broadcast_to(value, (8, LANES))[0:6] for value in coeffs]

    past_batches[1].arrived()

    first_set = sub < 4
    flat = jnp.zeros((8, LANES), F32)

    def write_feats(sx, s, tile_ref):
        whole = tile_ref[...]
        near = ends[sx, pl.ds(8 * s, 8), :]
        multipliers = []
        along = None
        for b in range(3):
            both = jnp.where(first_set, whole[b : b + 1], whole[4 + b : 5 + b])
            multipliers.append(both)
            term = near[b : b + 1] * both
            along = term if along is None else along + term
        multipliers.append(along)
        parts = [near * value for value in multipliers]
        for half_at in range(2):
            value = jnp.concatenate(parts[2 * half_at : 2 * half_at + 2], axis=0)
            for piece in range(3):
                kept = value.astype(BF16)
                feats[sx, s, pl.ds(32 * piece + 16 * half_at, 16), pl.ds(0, 128)] = kept
                value = value - kept.astype(F32)
        value = jnp.concatenate([flat, whole * (-1.0 / 3.0)], axis=0)
        for piece in range(3):
            kept = value.astype(BF16)
            feats[sx, s, pl.ds(32 * piece + 16, 16), pl.ds(128, 128)] = kept
            value = value - kept.astype(F32)

    def predict(sx, carry):
        for s in range(16):
            sy, sz = s // 4, s % 4
            value = None
            for h in range(5):
                term = coeffs[h] * past[sx, sy, sz, pl.ds(6 * h, 6), :]
                value = term if value is None else value + term
            moved_one[sx, sy, sz] = flat
            moved_one[sx, sy, sz, pl.ds(0, 3), :] = value[0:3]
            moved_one[sx, sy, sz, pl.ds(4, 3), :] = value[3:6]
        for s in range(16):
            write_feats(sx, s, moved_one.at[sx, s // 4, s % 4])
        return carry

    lax.fori_loop(0, 3, predict, 0)

    def dot_part(tile, sources):
        if len(sources) > 6:
            middle = len(sources) // 2
            return dot_piece(tile, sources[:middle]) + dot_piece(tile, sources[middle:])
        return dot_piece(tile, sources)

    def joined(summed):
        both = summed[:, 0:128] + summed[:, 128:256]
        return both[0:32] + both[32:64] + both[64:96]

    def dot_piece(tile, sources):
        ry, rz = RECEIVERS[tile]
        lhs = jnp.concatenate([feats[sx, 4 * sy + sz] for sx, sy, sz in sources], axis=1)
        rhs = jnp.concatenate(
            [pairs[tile, 9 * sx + 3 * (sy - ry) + sz - rz] for sx, sy, sz in sources], axis=0
        )
        return joined(jnp.dot(lhs, rhs, preferred_element_type=F32))

    def sources_of(tile, wanted=lambda source: True):
        ry, rz = RECEIVERS[tile]
        sources = [
            (sx, ry + ky, rz + kz) for sx in range(3) for ky in range(3) for kz in range(3)
        ]
        return [source for source in sources if wanted(source)]

    def relaxed(tile, before, out):
        ry, rz = RECEIVERS[tile]
        here = ends[1, pl.ds(8 * (4 * (ry + 1) + rz + 1), 8), :]
        value = out[24:32]
        for b in range(3):
            value = value - here[b : b + 1] * out[8 * b : 8 * b + 8]
        shared = jnp.where(first_set, value[3:4], value[7:8])
        field = value - here * shared
        return (1.0 - RELAXATION) * before + scaled_tiles[tile] * (perm_tiles[tile] + field)

    tile_batches = []
    summed = dot_part(0, sources_of(0))
    for tile, (ry, rz) in enumerate(RECEIVERS):
        now = summed
        if tile < 3:
            summed = dot_part(tile + 1, sources_of(tile + 1))
        before = moved_one[1, 1 + ry, 1 + rz]
        moved_two[1, 1 + ry, 1 + rz] = relaxed(tile, before, now)
        tile_batches.append(tile_batch(sizes, moved_two, sems[4 + tile], tile, counted.at[pl.ds(0, 11)]))
        tile_batches[-1].start()

    for batch in geo_batches + past_batches + [line_a, line_b, line_c]:
        batch.sent()

    own_sources = [(1, 1 + ry, 1 + rz) for ry, rz in RECEIVERS]

    def kind_of(source):
        return 2 * ((source[1] + 1) % 2) + (source[2] + 1) % 2

    for sx, sy, sz in own_sources:
        write_feats(sx, 4 * sy + sz, moved_two.at[sx, sy, sz])
    for tile in range(4):
        partial[tile] = dot_part(tile, own_sources)

    changed = flat
    size = flat
    for kinds in ((0, 1), (2, 3)):
        for kind in kinds:
            tile_batches[kind].arrived()

        def arriving(source):
            return kind_of(source) in kinds and source not in own_sources

        for source in [(sx, sy, sz) for sx in range(3) for sy in range(4) for sz in range(4)]:
            if arriving(source):
                sx, sy, sz = source
                write_feats(sx, 4 * sy + sz, moved_two.at[sx, sy, sz])
        for tile, (ry, rz) in enumerate(RECEIVERS):
            summed = partial[tile] + dot_part(tile, sources_of(tile, arriving))
            if kinds[-1] < 3:
                partial[tile] = summed
                continue
            before = moved_two[1, 1 + ry, 1 + rz]
            after = relaxed(tile, before, summed)
            out_ref[pl.ds(tile, 3, stride=4), :] = after[0:3]
            out_ref[pl.ds(12 + tile, 3, stride=4), :] = after[4:7]
            update = after - before
            changed = changed + update * update
            size = size + after * after

    def whole_sum(value):
        return jnp.sum(jnp.sum(value, axis=0, keepdims=True), axis=1, keepdims=True)

    row = jnp.where(lane == 0, whole_sum(changed), jnp.where(lane == 1, whole_sum(size), 0.0))
    ending = []
    for number in range(len(LAST_GROUPS)):
        ending.append(send_group(LAST_GROUPS, number, lines_two, 8 + len(FIRST_GROUPS), row))
        if number == 0:
            for batch in tile_batches:
                batch.sent()
        row = total(lines_two, number, ending[-1])
    top = jnp.sum(jnp.where(lane == 0, row, 0.0), axis=1, keepdims=True)
    bottom = jnp.sum(jnp.where(lane == 1, row, 0.0), axis=1, keepdims=True)
    change_ref[...] = jnp.broadcast_to(jnp.sqrt(top / (bottom + 1.0)), (1, LANES))

    for batch in ending:
        batch.sent()


def in_hbm(array):
    return pltpu.with_memory_space_constraint(array, pltpu.HBM)


def on_device(sizes, fractions, polarizability, occupancy, pair_mask, perm_field, history):
    vmem = pl.BlockSpec(memory_space=pltpu.VMEM)
    hbm = pl.BlockSpec(memory_space=pltpu.HBM)
    dma = pltpu.SemaphoreType.DMA
    line_bufs = [
        pltpu.VMEM((math.prod(sizes[axis] for axis in axes), 1, LANES), F32)
        for axes in FIRST_GROUPS + LAST_GROUPS
    ]
    scratch = [
        pltpu.VMEM((3, 4, LANES), F32),
        pltpu.VMEM((4, LANES), F32),
        pltpu.VMEM((4, LANES), jnp.int32),
        pltpu.SMEM((4, 27), jnp.int32),
        pltpu.VMEM((24, LANES), F32),
        pltpu.VMEM((6, 24, LANES), F32),
        pltpu.VMEM((4, 8, LANES), F32),
        pltpu.VMEM((3, 4, 4, 8, LANES), F32),
        pltpu.VMEM((3, 4, 4, 32, LANES), F32),
        pltpu.VMEM((6, 24, LANES), F32),
        pltpu.VMEM((3, 4, 4, 8, LANES), F32),
        pltpu.VMEM((3, 4, 4, 8, LANES), F32),
        pltpu.VMEM((4, 8, LANES), F32),
        pltpu.VMEM((4, 8, LANES), F32),
        pltpu.VMEM((32, LANES), F32),
        pltpu.VMEM((32, LANES), F32),
        pltpu.VMEM((3, LANES, LANES), F32),
        pltpu.VMEM((LANES, LANES), F32),
        pltpu.VMEM((LANES, LANES), F32),
        pltpu.VMEM((3, LANES, LANES), F32),
        pltpu.VMEM((4, 27, 256, 256), BF16),
        pltpu.VMEM((3, 16, 96, 256), BF16),
        pltpu.VMEM((4, 32, LANES), F32),
        pltpu.VMEM((28, 8, LANES), F32),
        dma((6,)),
        dma((SEMS,)),
        dma((SEMS,)),
    ]
    induced, change = pl.pallas_call(
        lambda *refs: kernel(sizes, *refs),
        out_shape=(
            jax.ShapeDtypeStruct((24, LANES), F32),
            jax.ShapeDtypeStruct((1, LANES), F32),
        ),
        in_specs=[hbm] * 6,
        out_specs=(vmem, vmem),
        scratch_shapes=scratch + line_bufs,
        compiler_params=pltpu.CompilerParams(
            collective_id=0, has_side_effects=True, vmem_limit_bytes=VMEM_BYTES
        ),
    )(
        in_hbm(fractions.reshape(3, 4, LANES)),
        in_hbm(polarizability.reshape(4, LANES)),
        in_hbm(occupancy.reshape(4, LANES)),
        in_hbm(pair_mask.reshape(4, 27)),
        in_hbm(perm_field.reshape(24, LANES)),
        in_hbm(history.reshape(6, 24, LANES)),
    )
    return induced.reshape(6, 1, 2, 2, LANES), change[0, 0]


def solution(mesh):
    sizes = {axis: mesh.shape[axis] for axis in AXES}
    placed = (
        P(None, "gx", "gy", "gz", None),
        P("gx", "gy", "gz", None),
        P("gx", "gy", "gz", None),
        P("gx", "gy", "gz", None),
        P(None, "gx", "gy", "gz", None),
        P(None, None, "gx", "gy", "gz", None),
    )
    return jax.shard_map(
        lambda *args: on_device(sizes, *args),
        mesh=mesh,
        in_specs=placed,
        out_specs=(P(None, "gx", "gy", "gz", None), P()),
        check_vma=False,
    )
```
